128 devices in a mesh: shard: 128 (over x, z, y, core).
Axes of the slice: x: 4, y: 4, z: 4, core: 2. Of those that a mesh axis runs over, the one named last changes fastest.
Arguments:
- lookup_ids: int32 [262144], P('shard'), may hold values from 0 to 2097151, as said below
- grad_rows: float32 [262144, 128], P('shard'), may hold values from -6 to 6
- emb_table: float32 [2097152, 128], P('shard'), may hold values from -4 to 4
- row_accum: float32 [2097152], P('shard'), may hold values from 0.01 to 1
Outputs:
- new_table: float32 [2097152, 128], P('shard')
- new_accum: float32 [2097152], P('shard')
- looked_up: float32 [262144, 128], P('shard')
The draws below stay inside these ranges and needn't reach their ends.
Inputs may be any that keep to these rules, and one draw needn't show every extreme that they name: `lookup_ids`: each device's 2048 lookups name exactly 16 rows, repeats counted, in the range of every owner; within an owner's range the row numbers follow a power law, so that a few rows are named very often.
All inputs are finite; a program needn't handle non-finite values.
Results may differ from the reference program's by a relative error of at most 0.00002.
Values sent between devices are 32-bit elements; how exact they have to be, the bound alone decides.
A program may use at most 64 MiB of HBM per device.

```python
import math
import jax
import jax.numpy as jnp
from jax import lax

W = 128
ROWS_DEV = 16384
LOOK_DEV = 2048
ROWS = 2097152
LOOKUPS = 262144
N_SHARD = 128


def draw_lookup_ids(key, part):
    key_perm, key_exp, key_row = jax.random.split(key, 3)
    perm_keys = jax.random.split(key_perm, N_SHARD)
    arrange = jax.vmap(lambda k: jax.random.permutation(k, LOOK_DEV))(perm_keys)
    owners = arrange % N_SHARD
    bit_count = ROWS_DEV.bit_length()
    exponent = jax.random.randint(key_exp, (N_SHARD, LOOK_DEV), 0, bit_count + 1)
    upper_limit = jnp.minimum(jnp.left_shift(jnp.ones_like(exponent), exponent), ROWS_DEV)
    local_rows = jax.random.randint(key_row, (N_SHARD, LOOK_DEV), 0, upper_limit)
    return (owners * ROWS_DEV + local_rows).reshape(-1).astype(jnp.int32)


def level_of(own_key, extent, cuts, low, largest):
    gain = 1.0
    for axis_at, parts in cuts:
        heights = jax.random.uniform(jax.random.fold_in(jax.random.fold_in(own_key, 6), axis_at), (parts,), jnp.float32, low / len(cuts), largest / len(cuts))
        gain = gain * jnp.repeat(jnp.exp(heights), extent[axis_at] // parts).reshape((-1,) + (1,) * (len(extent) - 1 - axis_at))
    return gain


def centred(own_key, dims, deviation, reach, shards=(), held_as=jnp.bfloat16):
    entries = deviation * jax.random.normal(own_key, dims, jnp.float32)
    if shards:
        entries = entries * level_of(own_key, dims, shards, -0.22, 0.18)
    return jnp.clip(entries, -reach, reach).astype(held_as)


def setup_inputs(seed: int = 0) -> dict:
    keys = jax.random.split(jax.random.key(seed), 5)
    return {
        "lookup_ids": draw_lookup_ids(jax.random.fold_in(keys[4], 71), 0),
        "grad_rows": centred(keys[1], (LOOKUPS, W), 1.0, 6.0, ((0, 128),), jnp.float32),
        "emb_table": centred(keys[2], (ROWS, W), 0.5, 4.0, ((0, 128),), jnp.float32),
        "row_accum": jnp.clip(jnp.exp(math.log(1.0) - 4.6051702 * jax.random.uniform(keys[3], (ROWS,), jnp.float32) ** level_of(keys[3], (ROWS,), ((0, 128),), -0.2, 0.2)), 0.01, 1.0),
    }


LEARNING_RATE = 0.5
EPSILON = 1e-08

def reference(lookup_ids, grad_rows, emb_table, row_accum):
    total_rows = emb_table.shape[0]
    summed = jax.ops.segment_sum(grad_rows, lookup_ids, num_segments=total_rows)
    new_accum = row_accum + lax.optimization_barrier(jnp.mean(summed * summed, axis=1))
    new_table = emb_table - LEARNING_RATE * summed / (jnp.sqrt(new_accum)[:, None] + EPSILON)
    looked_up = new_table[lookup_ids]
    return (new_table, new_accum, looked_up)
```

```python
import functools

import jax
import jax.numpy as jnp
from jax import lax
from jax.experimental import pallas as pl
from jax.experimental.pallas import tpu as pltpu
from jax.sharding import PartitionSpec as P

LEARNING_RATE = 0.5
EPSILON = 1e-08

MESH = pl.DeviceIdType.MESH
N = 128
W = 128
PER = 16
LOOK = N * PER
ROWS = 16384
ROW_BITS = 14
BLK = 128
NB = LOOK // BLK
SB = 256
NSB = LOOK // SB
PEERS_SB = SB // PER
F32, BF16, I32 = jnp.float32, jnp.bfloat16, jnp.int32


def iota(shape, dim):
    return lax.broadcasted_iota(I32, shape, dim)


def split2(x):
    hi = x.astype(BF16)
    return hi, (x - hi.astype(F32)).astype(BF16)


def onehot(mask):
    return jnp.where(mask, 1.0, 0.0).astype(BF16)


def mm(a, b):
    return jnp.dot(a, b, preferred_element_type=F32)


def mm_nt(a, b):
    return lax.dot_general(a, b, (((1,), (1,)), ((), ())), preferred_element_type=F32)


SLOT_OFFSETS = (1, 42, 84, 48, 8, 2, 4)


def offset_of(q):
    out = 0
    for i in range(4):
        if (q >> i) & 1:
            out ^= SLOT_OFFSETS[i]
    return out


def block_offset(t):
    return (t & 1) * 8 + ((t >> 1) & 1) * 2 + ((t >> 2) & 1) * 4


def slot_of(e):
    bit = lambda i: (e >> i) & 1
    q1 = bit(5) ^ bit(4) ^ bit(6)
    q = bit(0) + (q1 << 1) + (bit(6) << 2) + ((bit(4) ^ bit(6)) << 3)
    t = (bit(3) ^ q1) + ((bit(1) ^ q1) << 1) + ((bit(2) ^ bit(6)) << 2)
    return q + (t << 4)


def remote(src, dst, ssem, rsem, device):
    return pltpu.make_async_remote_copy(
        src_ref=src, dst_ref=dst, send_sem=ssem, recv_sem=rsem, device_id=(device,), device_id_type=MESH
    )


def exchange_kernel(
    ids_hbm, grads_hbm, accum_hbm, table_hbm,
    ret_ref, upd_ref, rows_ref, pos_ref, new_accum_ref, table,
    ids_ref, grads_ref, accum_ref, sendbuf, recvbuf, id_send, id_recv, split, eq, emb, rcol, acc_col, cnt_col,
    msq_col, rows_smem,
    id_ssem, id_rsem, g_ssem, g_rsem, r_ssem, r_rsem, smem_sem, in_sem,
):
    me = lax.axis_index("shard")
    barrier = pltpu.get_barrier_semaphore()

    def greet(k, c):
        pl.semaphore_signal(barrier, inc=1, device_id=(me ^ k,), device_id_type=MESH)
        return c

    lax.fori_loop(1, N, greet, 0)

    copies = [
        pltpu.make_async_copy(frm, to, in_sem.at[i])
        for i, (frm, to) in enumerate(
            ((ids_hbm, ids_ref), (grads_hbm, grads_ref), (accum_hbm, accum_ref), (table_hbm, table))
        )
    ]
    for copy in copies:
        copy.start()
    copies[0].wait()

    sub = iota((N, BLK), 0)
    lane = iota((N, BLK), 1)
    upper = onehot(sub <= lane)
    carry = jnp.zeros((N, 1), F32)
    w_hi = jnp.zeros((N, BLK), F32)
    w_lo = jnp.zeros((N, BLK), F32)
    for b in range(NB):
        ids = ids_ref[b : b + 1, :]
        slot = slot_of(lax.shift_right_logical(ids, ROW_BITS) ^ me)
        row = ids & (ROWS - 1)
        own = jnp.where(sub == slot, 1.0, 0.0)
        own_bf = own.astype(BF16)
        count = mm(own_bf, upper) + carry
        carry = carry + jnp.sum(own, axis=1, keepdims=True)
        rank = jnp.sum(own * count, axis=0, keepdims=True).astype(I32) - 1
        pos_ref[b : b + 1, :] = slot * PER + rank
        here = (sub & (PER - 1)) == rank
        q_hi = jnp.where(here, (row >> 7).astype(F32), 0.0).astype(BF16)
        q_lo = jnp.where(here, (row & 127).astype(F32), 0.0).astype(BF16)
        w_hi = w_hi + mm_nt(own_bf, q_hi)
        w_lo = w_lo + mm_nt(own_bf, q_lo)
    w = (w_hi.astype(I32) << 7) + w_lo.astype(I32)
    for d in range(N):
        id_send[d, 0:1, :] = w[d : d + 1, :]

    copies[1].wait()

    def split_grads(b, c):
        at = pl.ds(pl.multiple_of(b * SB, SB), SB)
        hi, lo = split2(grads_ref[at, :])
        split[at, 0:W] = hi
        split[at, W : 2 * W] = lo
        return c

    lax.fori_loop(0, NSB, split_grads, 0)

    def arrange(t, c):
        base = pl.multiple_of(t * SB, SB)
        want = iota((SB, BLK), 0) + base
        total = jnp.zeros((SB, 2 * W), F32)
        for b in range(NB):
            pick = onehot(want == pos_ref[b : b + 1, :])
            total = total + mm(pick, split[b * BLK : (b + 1) * BLK, :])
        sendbuf[pl.ds(base, SB), :] = total[:, 0:W] + total[:, W : 2 * W]
        return c

    lax.fori_loop(0, NSB, arrange, 0)

    def send_block(t, frm, to, ssem, rsem, first):
        far = me ^ block_offset(t)
        for q in range(first, PEERS_SB):
            slot = t * PEERS_SB + q
            remote(frm(slot), to(slot), ssem, rsem, far ^ offset_of(q)).start()

    def slot_rows(ref):
        return lambda slot: ref.at[pl.ds(pl.multiple_of(slot * PER, PER), PER)]

    def send_all(frm, to, ssem, rsem):
        send_block(0, frm, to, ssem, rsem, 1)

        def some(t, c):
            send_block(t, frm, to, ssem, rsem, 0)
            return c

        lax.fori_loop(1, NSB, some, 0)

    id_row = lambda ref: lambda slot: ref.at[slot, pl.ds(0, 1)]

    pl.semaphore_wait(barrier, N - 1)
    send_all(id_row(id_send), id_row(id_recv), id_ssem, id_rsem)
    send_all(slot_rows(sendbuf), slot_rows(recvbuf), g_ssem, g_rsem)
    id_recv[0, 0:1, :] = id_send[0, 0:1, :]
    recvbuf[0:PER, :] = sendbuf[0:PER, :]

    ids_all = remote(
        id_send.at[pl.ds(0, N - 1), pl.ds(0, 1)], id_recv.at[pl.ds(0, N - 1), pl.ds(0, 1)], id_ssem, id_rsem, me
    )
    ids_all.wait_send()
    ids_all.wait_recv()
    keep = (iota((8, BLK), 0) & 7) == (iota((8, BLK), 1) >> 4)
    for b in range(NB):
        got = jnp.concatenate([id_recv[8 * b + i, 0:1, :] for i in range(8)], axis=0)
        rows_ref[b : b + 1, :] = jnp.sum(jnp.where(keep, got, 0), axis=0, keepdims=True)
    to_smem = pltpu.make_async_copy(rows_ref, rows_smem, smem_sem)
    to_smem.start()
    for b in range(NB):
        row = rows_ref[b : b + 1, :].astype(F32)
        rcol[b * BLK : (b + 1) * BLK, :] = jnp.transpose(jnp.broadcast_to(row, (BLK, BLK)))

    copies[2].wait()
    acc_hi, acc_rest = split2(accum_ref[...])
    acc_lo = (accum_ref[...] - acc_hi.astype(F32) - acc_rest.astype(F32)).astype(BF16)
    acc3 = jnp.concatenate([acc_hi, acc_rest, acc_lo], axis=1)

    def build(b, c):
        at = pl.ds(pl.multiple_of(b * BLK, BLK), BLK)
        col = rcol[at, :]
        seen = jnp.zeros((BLK, BLK), F32)
        for o in range(NB):
            same = jnp.where(col == rows_ref[o : o + 1, :].astype(F32), 1.0, 0.0)
            seen = seen + same
            eq[at, o * BLK : (o + 1) * BLK] = same.astype(BF16)
        cnt_col[at, :] = jnp.broadcast_to(jnp.sum(seen, axis=1, keepdims=True), (BLK, BLK))
        num = col.astype(I32)
        lanes = iota((BLK, BLK), 1)
        picked = mm(onehot((num >> 7) == lanes), acc3)
        picked = picked[:, 0:W] + picked[:, W : 2 * W] + picked[:, 2 * W :]
        acc = jnp.sum(jnp.where((num & 127) == lanes, picked, 0.0), axis=1, keepdims=True)
        acc_col[at, :] = jnp.broadcast_to(acc, (BLK, BLK))
        return c

    lax.fori_loop(0, NB, build, 0)

    copies[3].wait()
    to_smem.wait()

    def gather(b, c):
        base = pl.multiple_of(b * BLK, BLK)
        for i in range(BLK):
            r = rows_smem[b, i] & (ROWS - 1)
            emb[pl.ds(base + i, 1), :] = table[pl.ds(r, 1), :]
        return c

    lax.fori_loop(0, NB, gather, 0)

    many = pl.ds(0, (N - 1) * PER)
    all_grads = remote(sendbuf.at[many], recvbuf.at[many], g_ssem, g_rsem, me)
    all_grads.wait_send()
    all_grads.wait_recv()

    def split_recv(b, c):
        at = pl.ds(pl.multiple_of(b * SB, SB), SB)
        hi, lo = split2(recvbuf[at, :])
        split[at, 0:W] = hi
        split[at, W : 2 * W] = lo
        return c

    lax.fori_loop(0, NSB, split_recv, 0)

    def update(t):
        at = pl.ds(pl.multiple_of(t * SB, SB), SB)
        both = mm(eq[at, :], split[...])
        summed = both[:, 0:W] + both[:, W : 2 * W]
        msq = jnp.broadcast_to(jnp.sum(summed * summed, axis=1, keepdims=True), (SB, W)) * (1.0 / W)
        msq_col[at, :] = msq
        upd_ref[at, :] = emb[at, :] - LEARNING_RATE * summed / (jnp.sqrt(acc_col[at, :] + msq) + EPSILON)

    def update_send(t, c):
        update(t)
        send_block(t, slot_rows(upd_ref), slot_rows(ret_ref), r_ssem, r_rsem, 0)
        return c

    update(0)
    send_block(0, slot_rows(upd_ref), slot_rows(ret_ref), r_ssem, r_rsem, 1)
    lax.fori_loop(1, NSB, update_send, 0)
    ret_ref[0:PER, :] = upd_ref[0:PER, :]

    delta = jnp.zeros((N, BLK), F32)
    for b in range(NB):
        at = slice(b * BLK, (b + 1) * BLK)
        lo_row = rcol[at, :].astype(I32) & 127
        term = jnp.where(lo_row == lane, msq_col[at, :] / cnt_col[at, :], 0.0)
        t_hi, t_mid = split2(term)
        t_lo = (term - t_hi.astype(F32) - t_mid.astype(F32)).astype(BF16)
        pick = onehot((rows_ref[b : b + 1, :] >> 7) == sub)
        delta = delta + mm(pick, t_hi) + mm(pick, t_mid) + mm(pick, t_lo)
    new_accum_ref[...] = accum_ref[...] + delta

    back = remote(upd_ref.at[many], ret_ref.at[many], r_ssem, r_rsem, me)
    back.wait_send()
    back.wait_recv()


def place_kernel(
    table_ref, upd_ref, ret_ref, rows_ref, pos_ref, accum_ref,
    new_table_ref, looked_ref, new_accum_ref, table,
    looked, sems,
):
    accum_out = pltpu.make_async_copy(accum_ref, new_accum_ref, sems.at[0])
    accum_out.start()

    def scatter(b, c):
        base = pl.multiple_of(b * BLK, BLK)
        for i in range(BLK):
            table[pl.ds(rows_ref[b, i], 1), :] = upd_ref[pl.ds(base + i, 1), :]
        return c

    lax.fori_loop(0, NB, scatter, 0)
    table_out = pltpu.make_async_copy(table, new_table_ref, sems.at[1])
    table_out.start()

    def unpermute(b, c):
        base = pl.multiple_of(b * BLK, BLK)
        for i in range(BLK):
            looked[pl.ds(base + i, 1), :] = ret_ref[pl.ds(pos_ref[b, i], 1), :]
        return c

    lax.fori_loop(0, NB, unpermute, 0)
    looked_out = pltpu.make_async_copy(looked, looked_ref, sems.at[2])
    looked_out.start()
    accum_out.wait()
    table_out.wait()
    looked_out.wait()


VM = pl.BlockSpec(memory_space=pltpu.VMEM)
SM = pl.BlockSpec(memory_space=pltpu.SMEM)
HBM = pl.BlockSpec(memory_space=pltpu.HBM)


def on_device(lookup_ids, grad_rows, emb_table, row_accum):
    dma = pltpu.SemaphoreType.DMA
    f32 = lambda *s: jax.ShapeDtypeStruct(s, F32)
    i32 = lambda *s: jax.ShapeDtypeStruct(s, I32)
    vmem = lambda *s: pltpu.VMEM(s, F32)
    in_hbm = lambda a: pltpu.with_memory_space_constraint(a, pltpu.HBM)
    ret, upd, rows, pos, stepped, held = pl.pallas_call(
        exchange_kernel,
        out_shape=(f32(LOOK, W), f32(LOOK, W), i32(NB, BLK), i32(NB, BLK), f32(N, BLK), vmem(ROWS, W)),
        in_specs=[HBM, HBM, HBM, HBM],
        out_specs=(VM, VM, VM, VM, VM, VM),
        scratch_shapes=[
            pltpu.VMEM((NB, BLK), I32),
            pltpu.VMEM((LOOK, W), F32),
            pltpu.VMEM((N, BLK), F32),
            pltpu.VMEM((LOOK, W), F32),
            pltpu.VMEM((LOOK, W), F32),
            pltpu.VMEM((N, 8, W), I32),
            pltpu.VMEM((N, 8, W), I32),
            pltpu.VMEM((LOOK, 2 * W), BF16),
            pltpu.VMEM((LOOK, LOOK), BF16),
            pltpu.VMEM((LOOK, W), F32),
            pltpu.VMEM((LOOK, W), F32),
            pltpu.VMEM((LOOK, W), F32),
            pltpu.VMEM((LOOK, W), F32),
            pltpu.VMEM((LOOK, W), F32),
            pltpu.SMEM((NB, BLK), I32),
            dma, dma, dma, dma, dma, dma, dma,
            pltpu.SemaphoreType.DMA((4,)),
        ],
        compiler_params=pltpu.CompilerParams(
            collective_id=0, has_side_effects=True, vmem_limit_bytes=28 * 1024 * 1024
        ),
    )(*map(in_hbm, (lookup_ids.reshape(NB, BLK), grad_rows, row_accum.reshape(N, BLK), emb_table)))
    new_table, looked_up, new_accum, _ = pl.pallas_call(
        place_kernel,
        out_shape=(f32(ROWS, W), f32(LOOK, W), f32(N, BLK), vmem(ROWS, W)),
        in_specs=[VM, VM, VM, SM, SM, VM],
        out_specs=(HBM, HBM, HBM, VM),
        input_output_aliases={0: 3},
        scratch_shapes=[pltpu.VMEM((LOOK, W), F32), pltpu.SemaphoreType.DMA((3,))],
        compiler_params=pltpu.CompilerParams(vmem_limit_bytes=4 * 1024 * 1024),
    )(held, upd, ret, rows, pos, stepped)
    return (new_table, new_accum.reshape(ROWS), looked_up)


def solution(mesh):
    in_specs = (P("shard"), P("shard", None), P("shard", None), P("shard"))
    out_specs = (P("shard", None), P("shard"), P("shard", None))
    return jax.shard_map(
        on_device, mesh=mesh, in_specs=in_specs, out_specs=out_specs, check_vma=False
    )
```

```python
import functools

import jax
import jax.numpy as jnp
from jax import lax
from jax.experimental import pallas as pl
from jax.experimental.pallas import tpu as pltpu
from jax.sharding import PartitionSpec as P

LEARNING_RATE = 0.5
EPSILON = 1e-08

MESH = pl.DeviceIdType.MESH
N = 128
W = 128
PER = 16
LOOK = N * PER
ROWS = 16384
ROW_BITS = 14
BLK = 128
NB = LOOK // BLK
SB = 256
NSB = LOOK // SB
PEERS_SB = SB // PER
F32, BF16, I32 = jnp.float32, jnp.bfloat16, jnp.int32


def iota(shape, dim):
    return lax.broadcasted_iota(I32, shape, dim)


def split2(x):
    hi = x.astype(BF16)
    return hi, (x - hi.astype(F32)).astype(BF16)


def onehot(mask):
    return jnp.where(mask, 1.0, 0.0).astype(BF16)


def mm(a, b):
    return jnp.dot(a, b, preferred_element_type=F32)


def mm_nt(a, b):
    return lax.dot_general(a, b, (((1,), (1,)), ((), ())), preferred_element_type=F32)


SLOT_OFFSETS = (1, 42, 84, 48, 8, 2, 4)


def offset_of(q):
    out = 0
    for i in range(4):
        if (q >> i) & 1:
            out ^= SLOT_OFFSETS[i]
    return out


def block_offset(t):
    return (t & 1) * 8 + ((t >> 1) & 1) * 2 + ((t >> 2) & 1) * 4


def slot_of(e):
    bit = lambda i: (e >> i) & 1
    q1 = bit(5) ^ bit(4) ^ bit(6)
    q = bit(0) + (q1 << 1) + (bit(6) << 2) + ((bit(4) ^ bit(6)) << 3)
    t = (bit(3) ^ q1) + ((bit(1) ^ q1) << 1) + ((bit(2) ^ bit(6)) << 2)
    return q + (t << 4)


def remote(src, dst, ssem, rsem, device):
    return pltpu.make_async_remote_copy(
        src_ref=src, dst_ref=dst, send_sem=ssem, recv_sem=rsem, device_id=(device,), device_id_type=MESH
    )


def exchange_kernel(
    ids_hbm, grads_hbm, accum_hbm, table_hbm,
    ret_ref, upd_ref, rows_ref, pos_ref, new_accum_ref, table,
    ids_ref, grads_ref, accum_ref, sendbuf, recvbuf, id_send, id_recv, split, eq, emb, rcol, acc_col, cnt_col,
    msq_col, rows_smem,
    id_ssem, id_rsem, g_ssem, g_rsem, r_ssem, r_rsem, smem_sem, in_sem,
):
    me = lax.axis_index("shard")
    barrier = pltpu.get_barrier_semaphore()

    def greet(k, c):
        pl.semaphore_signal(barrier, inc=1, device_id=(me ^ k,), device_id_type=MESH)
        return c

    lax.fori_loop(1, N, greet, 0)

    copies = [
        pltpu.make_async_copy(frm, to, in_sem.at[i])
        for i, (frm, to) in enumerate(
            ((ids_hbm, ids_ref), (grads_hbm, grads_ref), (accum_hbm, accum_ref), (table_hbm, table))
        )
    ]
    for copy in copies:
        copy.start()
    copies[0].wait()

    sub = iota((N, BLK), 0)
    lane = iota((N, BLK), 1)
    upper = onehot(sub <= lane)
    carry = jnp.zeros((N, 1), F32)
    w_hi = jnp.zeros((N, BLK), F32)
    w_lo = jnp.zeros((N, BLK), F32)
    for b in range(NB):
        ids = ids_ref[b : b + 1, :]
        slot = slot_of(lax.shift_right_logical(ids, ROW_BITS) ^ me)
        row = ids & (ROWS - 1)
        own = jnp.where(sub == slot, 1.0, 0.0)
        own_bf = own.astype(BF16)
        count = mm(own_bf, upper) + carry
        carry = carry + jnp.sum(own, axis=1, keepdims=True)
        rank = jnp.sum(own * count, axis=0, keepdims=True).astype(I32) - 1
        pos_ref[b : b + 1, :] = slot * PER + rank
        here = (sub & (PER - 1)) == rank
        q_hi = jnp.where(here, (row >> 7).astype(F32), 0.0).astype(BF16)
        q_lo = jnp.where(here, (row & 127).astype(F32), 0.0).astype(BF16)
        w_hi = w_hi + mm_nt(own_bf, q_hi)
        w_lo = w_lo + mm_nt(own_bf, q_lo)
    w = (w_hi.astype(I32) << 7) + w_lo.astype(I32)
    for d in range(N):
        id_send[d, 0:1, :] = w[d : d + 1, :]

    copies[1].wait()

    def split_grads(b, c):
        at = pl.ds(pl.multiple_of(b * SB, SB), SB)
        hi, lo = split2(grads_ref[at, :])
        split[at, 0:W] = hi
        split[at, W : 2 * W] = lo
        return c

    lax.fori_loop(0, NSB, split_grads, 0)

    def arrange(t):
        base = pl.multiple_of(t * SB, SB)
        want = iota((SB, BLK), 0) + base
        total = jnp.zeros((SB, 2 * W), F32)
        for b in range(NB):
            pick = onehot(want == pos_ref[b : b + 1, :])
            total = total + mm(pick, split[b * BLK : (b + 1) * BLK, :])
        sendbuf[pl.ds(base, SB), :] = total[:, 0:W] + total[:, W : 2 * W]

    def send_block(t, frm, to, ssem, rsem, first):
        far = me ^ block_offset(t)
        for q in range(first, PEERS_SB):
            slot = t * PEERS_SB + q
            remote(frm(slot), to(slot), ssem, rsem, far ^ offset_of(q)).start()

    def slot_rows(ref):
        return lambda slot: ref.at[pl.ds(pl.multiple_of(slot * PER, PER), PER)]

    def send_all(frm, to, ssem, rsem):
        send_block(0, frm, to, ssem, rsem, 1)

        def some(t, c):
            send_block(t, frm, to, ssem, rsem, 0)
            return c

        lax.fori_loop(1, NSB, some, 0)

    id_row = lambda ref: lambda slot: ref.at[slot, pl.ds(0, 1)]

    arrange(0)
    pl.semaphore_wait(barrier, N - 1)
    send_block(0, slot_rows(sendbuf), slot_rows(recvbuf), g_ssem, g_rsem, 1)
    send_all(id_row(id_send), id_row(id_recv), id_ssem, id_rsem)

    def arrange_send(t, c):
        arrange(t)
        send_block(t, slot_rows(sendbuf), slot_rows(recvbuf), g_ssem, g_rsem, 0)
        return c

    lax.fori_loop(1, NSB, arrange_send, 0)
    id_recv[0, 0:1, :] = id_send[0, 0:1, :]
    recvbuf[0:PER, :] = sendbuf[0:PER, :]

    ids_all = remote(
        id_send.at[pl.ds(0, N - 1), pl.ds(0, 1)], id_recv.at[pl.ds(0, N - 1), pl.ds(0, 1)], id_ssem, id_rsem, me
    )
    ids_all.wait_send()
    ids_all.wait_recv()
    keep = (iota((8, BLK), 0) & 7) == (iota((8, BLK), 1) >> 4)
    for b in range(NB):
        got = jnp.concatenate([id_recv[8 * b + i, 0:1, :] for i in range(8)], axis=0)
        rows_ref[b : b + 1, :] = jnp.sum(jnp.where(keep, got, 0), axis=0, keepdims=True)
    to_smem = pltpu.make_async_copy(rows_ref, rows_smem, smem_sem)
    to_smem.start()
    for b in range(NB):
        row = rows_ref[b : b + 1, :].astype(F32)
        rcol[b * BLK : (b + 1) * BLK, :] = jnp.transpose(jnp.broadcast_to(row, (BLK, BLK)))

    copies[2].wait()
    acc_hi, acc_rest = split2(accum_ref[...])
    acc_lo = (accum_ref[...] - acc_hi.astype(F32) - acc_rest.astype(F32)).astype(BF16)
    acc3 = jnp.concatenate([acc_hi, acc_rest, acc_lo], axis=1)

    def build(b, c):
        at = pl.ds(pl.multiple_of(b * BLK, BLK), BLK)
        col = rcol[at, :]
        seen = jnp.zeros((BLK, BLK), F32)
        for o in range(NB):
            same = jnp.where(col == rows_ref[o : o + 1, :].astype(F32), 1.0, 0.0)
            seen = seen + same
            eq[at, o * BLK : (o + 1) * BLK] = same.astype(BF16)
        cnt_col[at, :] = jnp.broadcast_to(jnp.sum(seen, axis=1, keepdims=True), (BLK, BLK))
        num = col.astype(I32)
        lanes = iota((BLK, BLK), 1)
        picked = mm(onehot((num >> 7) == lanes), acc3)
        picked = picked[:, 0:W] + picked[:, W : 2 * W] + picked[:, 2 * W :]
        acc = jnp.sum(jnp.where((num & 127) == lanes, picked, 0.0), axis=1, keepdims=True)
        acc_col[at, :] = jnp.broadcast_to(acc, (BLK, BLK))
        return c

    lax.fori_loop(0, NB, build, 0)

    copies[3].wait()
    to_smem.wait()

    def gather(b, c):
        base = pl.multiple_of(b * BLK, BLK)
        for i in range(BLK):
            r = rows_smem[b, i] & (ROWS - 1)
            emb[pl.ds(base + i, 1), :] = table[pl.ds(r, 1), :]
        return c

    lax.fori_loop(0, NB, gather, 0)

    many = pl.ds(0, (N - 1) * PER)
    all_grads = remote(sendbuf.at[many], recvbuf.at[many], g_ssem, g_rsem, me)
    all_grads.wait_send()
    all_grads.wait_recv()

    def split_recv(b, c):
        at = pl.ds(pl.multiple_of(b * SB, SB), SB)
        hi, lo = split2(recvbuf[at, :])
        split[at, 0:W] = hi
        split[at, W : 2 * W] = lo
        return c

    lax.fori_loop(0, NSB, split_recv, 0)

    def update(t):
        at = pl.ds(pl.multiple_of(t * SB, SB), SB)
        both = mm(eq[at, :], split[...])
        summed = both[:, 0:W] + both[:, W : 2 * W]
        msq = jnp.broadcast_to(jnp.sum(summed * summed, axis=1, keepdims=True), (SB, W)) * (1.0 / W)
        msq_col[at, :] = msq
        upd_ref[at, :] = emb[at, :] - LEARNING_RATE * summed / (jnp.sqrt(acc_col[at, :] + msq) + EPSILON)

    def update_send(t, c):
        update(t)
        send_block(t, slot_rows(upd_ref), slot_rows(ret_ref), r_ssem, r_rsem, 0)
        return c

    update(0)
    send_block(0, slot_rows(upd_ref), slot_rows(ret_ref), r_ssem, r_rsem, 1)
    lax.fori_loop(1, NSB, update_send, 0)
    ret_ref[0:PER, :] = upd_ref[0:PER, :]

    delta = jnp.zeros((N, BLK), F32)
    for b in range(NB):
        at = slice(b * BLK, (b + 1) * BLK)
        lo_row = rcol[at, :].astype(I32) & 127
        term = jnp.where(lo_row == lane, msq_col[at, :] / cnt_col[at, :], 0.0)
        t_hi, t_mid = split2(term)
        t_lo = (term - t_hi.astype(F32) - t_mid.astype(F32)).astype(BF16)
        pick = onehot((rows_ref[b : b + 1, :] >> 7) == sub)
        delta = delta + mm(pick, t_hi) + mm(pick, t_mid) + mm(pick, t_lo)
    new_accum_ref[...] = accum_ref[...] + delta

    back = remote(upd_ref.at[many], ret_ref.at[many], r_ssem, r_rsem, me)
    back.wait_send()
    back.wait_recv()


def place_kernel(
    table_ref, upd_ref, ret_ref, rows_ref, pos_ref, accum_ref,
    new_table_ref, looked_ref, new_accum_ref, table,
    looked, sems,
):
    accum_out = pltpu.make_async_copy(accum_ref, new_accum_ref, sems.at[0])
    accum_out.start()

    def scatter(b, c):
        base = pl.multiple_of(b * BLK, BLK)
        for i in range(BLK):
            table[pl.ds(rows_ref[b, i], 1), :] = upd_ref[pl.ds(base + i, 1), :]
        return c

    lax.fori_loop(0, NB, scatter, 0)
    table_out = pltpu.make_async_copy(table, new_table_ref, sems.at[1])
    table_out.start()

    def unpermute(b, c):
        base = pl.multiple_of(b * BLK, BLK)
        for i in range(BLK):
            looked[pl.ds(base + i, 1), :] = ret_ref[pl.ds(pos_ref[b, i], 1), :]
        return c

    lax.fori_loop(0, NB, unpermute, 0)
    looked_out = pltpu.make_async_copy(looked, looked_ref, sems.at[2])
    looked_out.start()
    accum_out.wait()
    table_out.wait()
    looked_out.wait()


VM = pl.BlockSpec(memory_space=pltpu.VMEM)
SM = pl.BlockSpec(memory_space=pltpu.SMEM)
HBM = pl.BlockSpec(memory_space=pltpu.HBM)


def on_device(lookup_ids, grad_rows, emb_table, row_accum):
    dma = pltpu.SemaphoreType.DMA
    f32 = lambda *s: jax.ShapeDtypeStruct(s, F32)
    i32 = lambda *s: jax.ShapeDtypeStruct(s, I32)
    vmem = lambda *s: pltpu.VMEM(s, F32)
    in_hbm = lambda a: pltpu.with_memory_space_constraint(a, pltpu.HBM)
    ret, upd, rows, pos, stepped, held = pl.pallas_call(
        exchange_kernel,
        out_shape=(f32(LOOK, W), f32(LOOK, W), i32(NB, BLK), i32(NB, BLK), f32(N, BLK), vmem(ROWS, W)),
        in_specs=[HBM, HBM, HBM, HBM],
        out_specs=(VM, VM, VM, VM, VM, VM),
        scratch_shapes=[
            pltpu.VMEM((NB, BLK), I32),
            pltpu.VMEM((LOOK, W), F32),
            pltpu.VMEM((N, BLK), F32),
            pltpu.VMEM((LOOK, W), F32),
            pltpu.VMEM((LOOK, W), F32),
            pltpu.VMEM((N, 8, W), I32),
            pltpu.VMEM((N, 8, W), I32),
            pltpu.VMEM((LOOK, 2 * W), BF16),
            pltpu.VMEM((LOOK, LOOK), BF16),
            pltpu.VMEM((LOOK, W), F32),
            pltpu.VMEM((LOOK, W), F32),
            pltpu.VMEM((LOOK, W), F32),
            pltpu.VMEM((LOOK, W), F32),
            pltpu.VMEM((LOOK, W), F32),
            pltpu.SMEM((NB, BLK), I32),
            dma, dma, dma, dma, dma, dma, dma,
            pltpu.SemaphoreType.DMA((4,)),
        ],
        compiler_params=pltpu.CompilerParams(
            collective_id=0, has_side_effects=True, vmem_limit_bytes=28 * 1024 * 1024
        ),
    )(*map(in_hbm, (lookup_ids.reshape(NB, BLK), grad_rows, row_accum.reshape(N, BLK), emb_table)))
    new_table, looked_up, new_accum, _ = pl.pallas_call(
        place_kernel,
        out_shape=(f32(ROWS, W), f32(LOOK, W), f32(N, BLK), vmem(ROWS, W)),
        in_specs=[VM, VM, VM, SM, SM, VM],
        out_specs=(HBM, HBM, HBM, VM),
        input_output_aliases={0: 3},
        scratch_shapes=[pltpu.VMEM((LOOK, W), F32), pltpu.SemaphoreType.DMA((3,))],
        compiler_params=pltpu.CompilerParams(vmem_limit_bytes=4 * 1024 * 1024),
    )(held, upd, ret, rows, pos, stepped)
    return (new_table, new_accum.reshape(ROWS), looked_up)


def solution(mesh):
    in_specs = (P("shard"), P("shard", None), P("shard", None), P("shard"))
    out_specs = (P("shard", None), P("shard"), P("shard", None))
    return jax.shard_map(
        on_device, mesh=mesh, in_specs=in_specs, out_specs=out_specs, check_vma=False
    )
```

```python
import functools

import jax
import jax.numpy as jnp
from jax import lax
from jax.experimental import pallas as pl
from jax.experimental.pallas import tpu as pltpu
from jax.sharding import PartitionSpec as P

LEARNING_RATE = 0.5
EPSILON = 1e-08

MESH = pl.DeviceIdType.MESH
N = 128
W = 128
PER = 16
LOOK = N * PER
ROWS = 16384
ROW_BITS = 14
BLK = 128
NB = LOOK // BLK
SB = 256
NSB = LOOK // SB
PEERS_SB = SB // PER
F32, BF16, I32 = jnp.float32, jnp.bfloat16, jnp.int32


def iota(shape, dim):
    return lax.broadcasted_iota(I32, shape, dim)


def split2(x):
    hi = x.astype(BF16)
    return hi, (x - hi.astype(F32)).astype(BF16)


def onehot(mask):
    return jnp.where(mask, 1.0, 0.0).astype(BF16)


def mm(a, b):
    return jnp.dot(a, b, preferred_element_type=F32)


def mm_nt(a, b):
    return lax.dot_general(a, b, (((1,), (1,)), ((), ())), preferred_element_type=F32)


SLOT_OFFSETS = (1, 42, 84, 48, 8, 2, 4)


def offset_of(q):
    out = 0
    for i in range(4):
        if (q >> i) & 1:
            out ^= SLOT_OFFSETS[i]
    return out


def block_offset(t):
    return (t & 1) * 8 + ((t >> 1) & 1) * 2 + ((t >> 2) & 1) * 4


def hops(k):
    return sum((0, 1, 2, 1)[(k >> i) & 3] for i in (1, 3, 5))


FAR_FIRST = sorted(range(1, N), key=lambda k: -hops(k))


def slot_of(e):
    bit = lambda i: (e >> i) & 1
    q1 = bit(5) ^ bit(4) ^ bit(6)
    q = bit(0) + (q1 << 1) + (bit(6) << 2) + ((bit(4) ^ bit(6)) << 3)
    t = (bit(3) ^ q1) + ((bit(1) ^ q1) << 1) + ((bit(2) ^ bit(6)) << 2)
    return q + (t << 4)


def remote(src, dst, ssem, rsem, device):
    return pltpu.make_async_remote_copy(
        src_ref=src, dst_ref=dst, send_sem=ssem, recv_sem=rsem, device_id=(device,), device_id_type=MESH
    )


def exchange_kernel(
    ids_hbm, grads_hbm, accum_hbm, table_hbm,
    ret_ref, upd_ref, rows_smem, pos_smem, new_accum_ref, table,
    rows_ref, pos_ref, first, ids_ref, grads_ref, accum_ref, sendbuf, recvbuf, id_send, id_recv, split, eq, emb, rcol, acc_col, cnt_col,
    msq_col,
    id_ssem, id_rsem, g_ssem, g_rsem, r_ssem, r_rsem, smem_sem, in_sem,
):
    me = lax.axis_index("shard")
    barrier = pltpu.get_barrier_semaphore()

    for k in FAR_FIRST:
        pl.semaphore_signal(barrier, inc=1, device_id=(me ^ k,), device_id_type=MESH)

    copies = [
        pltpu.make_async_copy(frm, to, in_sem.at[i])
        for i, (frm, to) in enumerate(
            ((ids_hbm, ids_ref), (grads_hbm, grads_ref), (accum_hbm, accum_ref), (table_hbm, table))
        )
    ]
    for copy in copies[:3]:
        copy.start()
    copies[0].wait()

    sub = iota((N, BLK), 0)
    lane = iota((N, BLK), 1)
    upper = onehot(sub <= lane)
    carry = jnp.zeros((N, 1), F32)

    def slots_at(b):
        return slot_of(lax.shift_right_logical(ids_ref[b : b + 1, :], ROW_BITS) ^ me)

    for b in range(NB):
        slot = slots_at(b)
        own = jnp.where(sub == slot, 1.0, 0.0)
        count = mm(own.astype(BF16), upper) + carry
        carry = carry + jnp.sum(own, axis=1, keepdims=True)
        rank = jnp.sum(own * count, axis=0, keepdims=True).astype(I32) - 1
        pos_ref[b : b + 1, :] = slot * PER + rank

    def pack_ids():
        w_hi = jnp.zeros((N, BLK), F32)
        w_lo = jnp.zeros((N, BLK), F32)
        for b in range(NB):
            pos = pos_ref[b : b + 1, :]
            row = ids_ref[b : b + 1, :] & (ROWS - 1)
            own = onehot(sub == lax.shift_right_logical(pos, 4))
            here = (sub & (PER - 1)) == (pos & (PER - 1))
            q_hi = jnp.where(here, (row >> 7).astype(F32), 0.0).astype(BF16)
            q_lo = jnp.where(here, (row & 127).astype(F32), 0.0).astype(BF16)
            w_hi = w_hi + mm_nt(own, q_hi)
            w_lo = w_lo + mm_nt(own, q_lo)
        w = (w_hi.astype(I32) << 7) + w_lo.astype(I32)
        for d in range(N):
            id_send[d, 0:1, :] = w[d : d + 1, :]

    copies[1].wait()
    copies[3].start()

    def split_grads(b, c):
        at = pl.ds(pl.multiple_of(b * SB, SB), SB)
        hi, lo = split2(grads_ref[at, :])
        split[at, 0:W] = hi
        split[at, W : 2 * W] = lo
        return c

    lax.fori_loop(0, NSB, split_grads, 0)

    def arrange(t):
        base = pl.multiple_of(t * SB, SB)
        want = iota((SB, BLK), 0) + base
        total = jnp.zeros((SB, 2 * W), F32)
        for b in range(NB):
            pick = onehot(want == pos_ref[b : b + 1, :])
            total = total + mm(pick, split[b * BLK : (b + 1) * BLK, :])
        sendbuf[pl.ds(base, SB), :] = total[:, 0:W] + total[:, W : 2 * W]

    def send_block(t, frm, to, ssem, rsem, first):
        far = me ^ block_offset(t)
        for q in range(first, PEERS_SB):
            slot = t * PEERS_SB + q
            remote(frm(slot), to(slot), ssem, rsem, far ^ offset_of(q)).start()

    def slot_rows(ref):
        return lambda slot: ref.at[pl.ds(pl.multiple_of(slot * PER, PER), PER)]

    def send_all(frm, to, ssem, rsem):
        send_block(0, frm, to, ssem, rsem, 1)

        def some(t, c):
            send_block(t, frm, to, ssem, rsem, 0)
            return c

        lax.fori_loop(1, NSB, some, 0)

    id_row = lambda ref: lambda slot: ref.at[slot, pl.ds(0, 1)]

    arrange(0)
    pl.semaphore_wait(barrier, N - 1)
    send_block(0, slot_rows(sendbuf), slot_rows(recvbuf), g_ssem, g_rsem.at[0], 1)
    pack_ids()
    send_all(id_row(id_send), id_row(id_recv), id_ssem, id_rsem)

    def arrange_send(t, c):
        arrange(t)
        send_block(t, slot_rows(sendbuf), slot_rows(recvbuf), g_ssem, g_rsem.at[t], 0)
        return c

    lax.fori_loop(1, NSB, arrange_send, 0)
    to_smem = [
        pltpu.make_async_copy(frm, to, smem_sem.at[i])
        for i, (frm, to) in enumerate(((pos_ref, pos_smem), (rows_ref, rows_smem)))
    ]
    to_smem[0].start()
    id_recv[0, 0:1, :] = id_send[0, 0:1, :]
    recvbuf[0:PER, :] = sendbuf[0:PER, :]

    ids_all = remote(
        id_send.at[pl.ds(0, N - 1), pl.ds(0, 1)], id_recv.at[pl.ds(0, N - 1), pl.ds(0, 1)], id_ssem, id_rsem, me
    )
    ids_all.wait_send()
    ids_all.wait_recv()
    keep = (iota((8, BLK), 0) & 7) == (iota((8, BLK), 1) >> 4)
    for b in range(NB):
        got = jnp.concatenate([id_recv[8 * b + i, 0:1, :] for i in range(8)], axis=0)
        rows_ref[b : b + 1, :] = jnp.sum(jnp.where(keep, got, 0), axis=0, keepdims=True)
    to_smem[1].start()
    for b in range(NB):
        row = rows_ref[b : b + 1, :].astype(F32)
        rcol[b * BLK : (b + 1) * BLK, :] = jnp.transpose(jnp.broadcast_to(row, (BLK, BLK)))

    copies[2].wait()
    acc_hi, acc_rest = split2(accum_ref[...])
    acc_lo = (accum_ref[...] - acc_hi.astype(F32) - acc_rest.astype(F32)).astype(BF16)
    acc3 = jnp.concatenate([acc_hi, acc_rest, acc_lo], axis=1)

    def build(b, c):
        at = pl.ds(pl.multiple_of(b * BLK, BLK), BLK)
        col = rcol[at, :]
        seen = jnp.zeros((BLK, BLK), F32)
        for o in range(NB):
            same = jnp.where(col == rows_ref[o : o + 1, :].astype(F32), 1.0, 0.0)
            seen = seen + same
            eq[at, o * BLK : (o + 1) * BLK] = same.astype(BF16)
        cnt_col[at, :] = jnp.broadcast_to(jnp.sum(seen, axis=1, keepdims=True), (BLK, BLK))
        num = col.astype(I32)
        lanes = iota((BLK, BLK), 1)
        picked = mm(onehot((num >> 7) == lanes), acc3)
        picked = picked[:, 0:W] + picked[:, W : 2 * W] + picked[:, 2 * W :]
        acc = jnp.sum(jnp.where((num & 127) == lanes, picked, 0.0), axis=1, keepdims=True)
        acc_col[at, :] = jnp.broadcast_to(acc, (BLK, BLK))
        return c

    lax.fori_loop(0, NB, build, 0)

    copies[3].wait()
    to_smem[0].wait()
    to_smem[1].wait()

    def gather(b, c):
        base = pl.multiple_of(b * BLK, BLK)
        for i in range(BLK):
            r = rows_smem[b, i] & (ROWS - 1)
            emb[pl.ds(base + i, 1), :] = table[pl.ds(r, 1), :]
        return c

    lax.fori_loop(0, NB, gather, 0)

    def split_recv(t):
        at = pl.ds(pl.multiple_of(t * SB, SB), SB)
        hi, lo = split2(recvbuf[at, :])
        split[at, 0:W] = hi
        split[at, W : 2 * W] = lo
        return mm(eq[0:SB, at], split[at, :])

    def arrived(lo, rows, sem):
        at = pl.ds(lo, rows)
        remote(sendbuf.at[at], recvbuf.at[at], g_ssem, sem, me).wait_recv()

    arrived(PER, SB - PER, g_rsem.at[0])
    first[...] = split_recv(0)

    def take(t, c):
        arrived(pl.multiple_of(t * SB, SB), SB, g_rsem.at[t])
        first[...] += split_recv(t)
        return c

    lax.fori_loop(1, NSB, take, 0)

    def update(t, both):
        at = pl.ds(pl.multiple_of(t * SB, SB), SB)
        summed = both[:, 0:W] + both[:, W : 2 * W]
        msq = jnp.broadcast_to(jnp.sum(summed * summed, axis=1, keepdims=True), (SB, W)) * (1.0 / W)
        msq_col[at, :] = msq
        upd_ref[at, :] = emb[at, :] - LEARNING_RATE * summed / (jnp.sqrt(acc_col[at, :] + msq) + EPSILON)

    def update_send(t, c):
        update(t, mm(eq[pl.ds(pl.multiple_of(t * SB, SB), SB), :], split[...]))
        send_block(t, slot_rows(upd_ref), slot_rows(ret_ref), r_ssem, r_rsem, 0)
        return c

    update(0, first[...])
    send_block(0, slot_rows(upd_ref), slot_rows(ret_ref), r_ssem, r_rsem, 1)
    lax.fori_loop(1, NSB, update_send, 0)
    ret_ref[0:PER, :] = upd_ref[0:PER, :]

    delta = jnp.zeros((N, BLK), F32)
    for b in range(NB):
        at = slice(b * BLK, (b + 1) * BLK)
        lo_row = rcol[at, :].astype(I32) & 127
        term = jnp.where(lo_row == lane, msq_col[at, :] / cnt_col[at, :], 0.0)
        t_hi, t_mid = split2(term)
        t_lo = (term - t_hi.astype(F32) - t_mid.astype(F32)).astype(BF16)
        pick = onehot((rows_ref[b : b + 1, :] >> 7) == sub)
        delta = delta + mm(pick, t_hi) + mm(pick, t_mid) + mm(pick, t_lo)
    new_accum_ref[...] = accum_ref[...] + delta

    many = pl.ds(0, (N - 1) * PER)
    remote(sendbuf.at[many], recvbuf.at[many], g_ssem, g_rsem.at[0], me).wait_send()
    back = remote(upd_ref.at[many], ret_ref.at[many], r_ssem, r_rsem, me)
    back.wait_send()
    back.wait_recv()


def place_kernel(
    table_ref, upd_ref, ret_ref, rows_ref, pos_ref, accum_ref,
    new_table_ref, looked_ref, new_accum_ref, table,
    looked, sems,
):
    accum_out = pltpu.make_async_copy(accum_ref, new_accum_ref, sems.at[0])
    accum_out.start()

    def scatter(b, c):
        base = pl.multiple_of(b * BLK, BLK)
        for i in range(BLK):
            table[pl.ds(rows_ref[b, i], 1), :] = upd_ref[pl.ds(base + i, 1), :]
        return c

    lax.fori_loop(0, NB, scatter, 0)
    table_out = pltpu.make_async_copy(table, new_table_ref, sems.at[1])
    table_out.start()

    def unpermute(b, c):
        base = pl.multiple_of(b * BLK, BLK)
        for i in range(BLK):
            looked[pl.ds(base + i, 1), :] = ret_ref[pl.ds(pos_ref[b, i], 1), :]
        return c

    lax.fori_loop(0, NB, unpermute, 0)
    looked_out = pltpu.make_async_copy(looked, looked_ref, sems.at[2])
    looked_out.start()
    accum_out.wait()
    table_out.wait()
    looked_out.wait()


VM = pl.BlockSpec(memory_space=pltpu.VMEM)
SM = pl.BlockSpec(memory_space=pltpu.SMEM)
HBM = pl.BlockSpec(memory_space=pltpu.HBM)


def on_device(lookup_ids, grad_rows, emb_table, row_accum):
    dma = pltpu.SemaphoreType.DMA
    f32 = lambda *s: jax.ShapeDtypeStruct(s, F32)
    smem = lambda *s: pltpu.SMEM(s, I32)
    vmem = lambda *s: pltpu.VMEM(s, F32)
    in_hbm = lambda a: pltpu.with_memory_space_constraint(a, pltpu.HBM)
    ret, upd, rows, pos, stepped, held = pl.pallas_call(
        exchange_kernel,
        out_shape=(f32(LOOK, W), f32(LOOK, W), smem(NB, BLK), smem(NB, BLK), f32(N, BLK), vmem(ROWS, W)),
        in_specs=[HBM, HBM, HBM, HBM],
        out_specs=(VM, VM, SM, SM, VM, VM),
        scratch_shapes=[
            pltpu.VMEM((NB, BLK), I32),
            pltpu.VMEM((NB, BLK), I32),
            pltpu.VMEM((SB, 2 * W), F32),
            pltpu.VMEM((NB, BLK), I32),
            pltpu.VMEM((LOOK, W), F32),
            pltpu.VMEM((N, BLK), F32),
            pltpu.VMEM((LOOK, W), F32),
            pltpu.VMEM((LOOK, W), F32),
            pltpu.VMEM((N, 8, W), I32),
            pltpu.VMEM((N, 8, W), I32),
            pltpu.VMEM((LOOK, 2 * W), BF16),
            pltpu.VMEM((LOOK, LOOK), BF16),
            pltpu.VMEM((LOOK, W), F32),
            pltpu.VMEM((LOOK, W), F32),
            pltpu.VMEM((LOOK, W), F32),
            pltpu.VMEM((LOOK, W), F32),
            pltpu.VMEM((LOOK, W), F32),
            dma, dma, dma, pltpu.SemaphoreType.DMA((NSB,)), dma, dma,
            pltpu.SemaphoreType.DMA((2,)), pltpu.SemaphoreType.DMA((4,)),
        ],
        compiler_params=pltpu.CompilerParams(
            collective_id=0, has_side_effects=True, vmem_limit_bytes=28 * 1024 * 1024
        ),
    )(*map(in_hbm, (lookup_ids.reshape(NB, BLK), grad_rows, row_accum.reshape(N, BLK), emb_table)))
    new_table, looked_up, new_accum, _ = pl.pallas_call(
        place_kernel,
        out_shape=(f32(ROWS, W), f32(LOOK, W), f32(N, BLK), vmem(ROWS, W)),
        in_specs=[VM, VM, VM, SM, SM, VM],
        out_specs=(HBM, HBM, HBM, VM),
        input_output_aliases={0: 3},
        scratch_shapes=[pltpu.VMEM((LOOK, W), F32), pltpu.SemaphoreType.DMA((3,))],
        compiler_params=pltpu.CompilerParams(vmem_limit_bytes=4 * 1024 * 1024),
    )(held, upd, ret, rows, pos, stepped)
    return (new_table, new_accum.reshape(ROWS), looked_up)


def solution(mesh):
    in_specs = (P("shard"), P("shard", None), P("shard", None), P("shard"))
    out_specs = (P("shard", None), P("shard"), P("shard", None))
    return jax.shard_map(
        on_device, mesh=mesh, in_specs=in_specs, out_specs=out_specs, check_vma=False
    )
```

```python
import functools

import jax
import jax.numpy as jnp
from jax import lax
from jax.experimental import pallas as pl
from jax.experimental.pallas import tpu as pltpu
from jax.sharding import PartitionSpec as P

LEARNING_RATE = 0.5
EPSILON = 1e-08

MESH = pl.DeviceIdType.MESH
N = 128
W = 128
PER = 16
LOOK = N * PER
ROWS = 16384
ROW_BITS = 14
BLK = 128
NB = LOOK // BLK
SB = 256
NSB = LOOK // SB
PEERS_SB = SB // PER
F32, BF16, I32 = jnp.float32, jnp.bfloat16, jnp.int32


def iota(shape, dim):
    return lax.broadcasted_iota(I32, shape, dim)


def split2(x):
    hi = x.astype(BF16)
    return hi, (x - hi.astype(F32)).astype(BF16)


def onehot(mask):
    return jnp.where(mask, 1.0, 0.0).astype(BF16)


def mm(a, b):
    return jnp.dot(a, b, preferred_element_type=F32)


def mm_nt(a, b):
    return lax.dot_general(a, b, (((1,), (1,)), ((), ())), preferred_element_type=F32)


def hops(k):
    return sum((0, 1, 2, 1)[(k >> i) & 3] for i in (1, 3, 5))


OFFSETS = sorted(range(1, N), key=lambda k: (-hops(k), -(k & 1), k >> 5)) + [0]
SELF = N - 1
PICK = 512
IDS_AT = 1


def remote(src, dst, ssem, rsem, device):
    return pltpu.make_async_remote_copy(
        src_ref=src, dst_ref=dst, send_sem=ssem, recv_sem=rsem, device_id=(device,), device_id_type=MESH
    )


def exchange_kernel(
    ids_hbm, grads_hbm, accum_hbm, table_hbm,
    ret_ref, upd_ref, rows_smem, pos_smem, new_accum_ref, table,
    rows_ref, pos_ref, first, ids_ref, grads_ref, accum_ref, sendbuf, recvbuf, id_send, id_recv, split, eq, emb, rcol, acc_col, start_at,
    msq_col,
    id_ssem, id_rsem, g_ssem, g_rsem, r_ssem, r_rsem, smem_sem, in_sem,
):
    me = lax.axis_index("shard")
    barrier = pltpu.get_barrier_semaphore()

    for k in OFFSETS[:SELF]:
        pl.semaphore_signal(barrier, inc=1, device_id=(me ^ k,), device_id_type=MESH)

    copies = [
        pltpu.make_async_copy(frm, to, in_sem.at[i])
        for i, (frm, to) in enumerate(
            ((ids_hbm, ids_ref), (grads_hbm, grads_ref), (accum_hbm, accum_ref), (table_hbm, table))
        )
    ]
    for copy in copies[:3]:
        copy.start()

    sub = iota((N, BLK), 0)
    lane = iota((N, BLK), 1)
    upper = onehot(sub <= lane)
    for k in range(N):
        start_at[k : k + 1, :] = jnp.full((1, BLK), float(OFFSETS.index(k) * PER - 1), F32)
    copies[0].wait()
    carry = start_at[...]
    for b in range(NB):
        peer = lax.shift_right_logical(ids_ref[b : b + 1, :], ROW_BITS) ^ me
        own = jnp.where(sub == peer, 1.0, 0.0)
        place = mm(own.astype(BF16), upper) + carry
        carry = carry + jnp.sum(own, axis=1, keepdims=True)
        pos_ref[b : b + 1, :] = jnp.sum(own * place, axis=0, keepdims=True).astype(I32)

    def pack_ids():
        w_hi = jnp.zeros((N, BLK), F32)
        w_lo = jnp.zeros((N, BLK), F32)
        for b in range(NB):
            pos = pos_ref[b : b + 1, :]
            row = ids_ref[b : b + 1, :] & (ROWS - 1)
            own = onehot(sub == lax.shift_right_logical(pos, 4))
            here = (sub & (PER - 1)) == (pos & (PER - 1))
            q_hi = jnp.where(here, (row >> 7).astype(F32), 0.0).astype(BF16)
            q_lo = jnp.where(here, (row & 127).astype(F32), 0.0).astype(BF16)
            w_hi = w_hi + mm_nt(own, q_hi)
            w_lo = w_lo + mm_nt(own, q_lo)
        w = (w_hi.astype(I32) << 7) + w_lo.astype(I32)
        for d in range(N):
            id_send[d, 0:1, :] = w[d : d + 1, :]

    copies[1].wait()
    copies[3].start()

    def split_grads(b, c):
        at = pl.ds(pl.multiple_of(b * SB, SB), SB)
        hi, lo = split2(grads_ref[at, :])
        split[at, 0:W] = hi
        split[at, W : 2 * W] = lo
        return c

    lax.fori_loop(0, NSB, split_grads, 0)

    def arrange(t):
        base = pl.multiple_of(t * SB, SB)
        want = iota((SB, BLK), 0) + base
        total = jnp.zeros((SB, 2 * W), F32)
        for b in range(NB):
            pick = onehot(want == pos_ref[b : b + 1, :])
            total = total + mm(pick, split[b * BLK : (b + 1) * BLK, :])
        sendbuf[pl.ds(base, SB), :] = total[:, 0:W] + total[:, W : 2 * W]

    def send_block(t, frm, to, ssem, rsem):
        for q in range(PEERS_SB):
            slot = t * PEERS_SB + q
            if slot != SELF:
                remote(frm(slot), to(slot), ssem, rsem, me ^ OFFSETS[slot]).start()

    def send_block_at(t, *how):
        for block in range(NSB):

            @pl.when(t == block)
            def _():
                send_block(block, *how)

    def slot_rows(ref):
        return lambda slot: ref.at[pl.ds(slot * PER, PER)]

    id_row = lambda ref: lambda slot: ref.at[slot, pl.ds(0, 1)]

    arrange(0)
    pl.semaphore_wait(barrier, N - 1)
    send_block(0, slot_rows(sendbuf), slot_rows(recvbuf), g_ssem, g_rsem.at[0])

    def arrange_send(t, c):
        arrange(t)
        send_block_at(t, slot_rows(sendbuf), slot_rows(recvbuf), g_ssem, g_rsem.at[t])
        return c

    lax.fori_loop(1, IDS_AT, arrange_send, 0)
    pack_ids()
    for t in range(NSB):
        send_block(t, id_row(id_send), id_row(id_recv), id_ssem, id_rsem)
    lax.fori_loop(IDS_AT, NSB, arrange_send, 0)
    id_recv[SELF, 0:1, :] = id_send[SELF, 0:1, :]
    recvbuf[SELF * PER :, :] = sendbuf[SELF * PER :, :]
    to_smem = [
        pltpu.make_async_copy(frm, to, smem_sem.at[i])
        for i, (frm, to) in enumerate(((pos_ref, pos_smem), (rows_ref, rows_smem)))
    ]
    to_smem[0].start()

    ids_all = remote(
        id_send.at[pl.ds(0, N - 1), pl.ds(0, 1)], id_recv.at[pl.ds(0, N - 1), pl.ds(0, 1)], id_ssem, id_rsem, me
    )
    ids_all.wait_send()
    ids_all.wait_recv()
    keep = (iota((8, BLK), 0) & 7) == (iota((8, BLK), 1) >> 4)
    for b in range(NB):
        got = jnp.concatenate([id_recv[8 * b + i, 0:1, :] for i in range(8)], axis=0)
        rows_ref[b : b + 1, :] = jnp.sum(jnp.where(keep, got, 0), axis=0, keepdims=True)
    to_smem[1].start()
    for b in range(NB):
        row = rows_ref[b : b + 1, :].astype(F32)
        rcol[b * BLK : (b + 1) * BLK, :] = jnp.transpose(jnp.broadcast_to(row, (BLK, BLK)))

    copies[2].wait()
    def build(b, c):
        at = pl.ds(pl.multiple_of(b * BLK, BLK), BLK)
        col = rcol[at, :]
        for o in range(NB):
            same = jnp.where(col == rows_ref[o : o + 1, :].astype(F32), 1.0, 0.0)
            eq[at, o * BLK : (o + 1) * BLK] = same.astype(BF16)
        return c

    lax.fori_loop(0, NB, build, 0)

    acc_hi, acc_rest = split2(accum_ref[...])
    acc_lo = (accum_ref[...] - acc_hi.astype(F32) - acc_rest.astype(F32)).astype(BF16)
    acc3 = jnp.concatenate([acc_hi, acc_rest, acc_lo], axis=1)

    def pick_accum(b, c):
        at = pl.ds(pl.multiple_of(b * PICK, PICK), PICK)
        num = rcol[at, :].astype(I32)
        lanes = iota((PICK, BLK), 1)
        picked = mm(onehot((num >> 7) == lanes), acc3)
        picked = picked[:, 0:W] + picked[:, W : 2 * W] + picked[:, 2 * W :]
        acc = jnp.sum(jnp.where((num & 127) == lanes, picked, 0.0), axis=1, keepdims=True)
        acc_col[at, :] = jnp.broadcast_to(acc, (PICK, BLK))
        return c

    lax.fori_loop(0, LOOK // PICK, pick_accum, 0)

    copies[3].wait()
    to_smem[0].wait()
    to_smem[1].wait()

    def gather(t):
        for h in range(SB // BLK):
            base = pl.multiple_of(t * SB + h * BLK, BLK)
            for i in range(BLK):
                r = rows_smem[t * (SB // BLK) + h, i] & (ROWS - 1)
                emb[pl.ds(base + i, 1), :] = table[pl.ds(r, 1), :]

    gather(0)

    def split_recv(t):
        at = pl.ds(pl.multiple_of(t * SB, SB), SB)
        hi, lo = split2(recvbuf[at, :])
        split[at, 0:W] = hi
        split[at, W : 2 * W] = lo
        return mm(eq[0:SB, at], split[at, :])

    def arrived(lo, rows, sem):
        at = pl.ds(lo, rows)
        remote(sendbuf.at[at], recvbuf.at[at], g_ssem, sem, me).wait_recv()

    arrived(0, SB, g_rsem.at[0])
    first[...] = split_recv(0)

    def take(t, c):
        arrived(pl.multiple_of(t * SB, SB), SB, g_rsem.at[t])
        first[...] += split_recv(t)
        return c

    lax.fori_loop(1, NSB - 1, take, 0)
    arrived((NSB - 1) * SB, SB - PER, g_rsem.at[NSB - 1])
    first[...] += split_recv(NSB - 1)

    def update(t, both):
        at = pl.ds(pl.multiple_of(t * SB, SB), SB)
        summed = both[:, 0:W] + both[:, W : 2 * W]
        msq = jnp.broadcast_to(jnp.sum(summed * summed, axis=1, keepdims=True), (SB, W)) * (1.0 / W)
        msq_col[at, :] = msq
        upd_ref[at, :] = emb[at, :] - LEARNING_RATE * summed / (jnp.sqrt(acc_col[at, :] + msq) + EPSILON)

    def update_send(t, c):
        gather(t)
        update(t, mm(eq[pl.ds(pl.multiple_of(t * SB, SB), SB), :], split[...]))
        send_block_at(t, slot_rows(upd_ref), slot_rows(ret_ref), r_ssem, r_rsem)
        return c

    update(0, first[...])
    send_block(0, slot_rows(upd_ref), slot_rows(ret_ref), r_ssem, r_rsem)
    lax.fori_loop(1, NSB, update_send, 0)
    ret_ref[SELF * PER :, :] = upd_ref[SELF * PER :, :]

    delta = jnp.zeros((N, BLK), F32)
    for b in range(NB):
        at = slice(b * BLK, (b + 1) * BLK)
        lo_row = rcol[at, :].astype(I32) & 127
        count = mm(eq[at, :], jnp.ones((LOOK, BLK), BF16))
        term = jnp.where(lo_row == lane, msq_col[at, :] / count, 0.0)
        t_hi, t_mid = split2(term)
        t_lo = (term - t_hi.astype(F32) - t_mid.astype(F32)).astype(BF16)
        pick = onehot((rows_ref[b : b + 1, :] >> 7) == sub)
        delta = delta + mm(pick, t_hi) + mm(pick, t_mid) + mm(pick, t_lo)
    new_accum_ref[...] = accum_ref[...] + delta

    many = pl.ds(0, (N - 1) * PER)
    remote(sendbuf.at[many], recvbuf.at[many], g_ssem, g_rsem.at[0], me).wait_send()
    back = remote(upd_ref.at[many], ret_ref.at[many], r_ssem, r_rsem, me)
    back.wait_send()
    back.wait_recv()


def place_kernel(
    table_ref, upd_ref, ret_ref, rows_ref, pos_ref, accum_ref,
    new_table_ref, looked_ref, new_accum_ref, table,
    looked, sems,
):
    accum_out = pltpu.make_async_copy(accum_ref, new_accum_ref, sems.at[0])
    accum_out.start()

    def scatter(b, c):
        base = pl.multiple_of(b * BLK, BLK)
        for i in range(BLK):
            table[pl.ds(rows_ref[b, i], 1), :] = upd_ref[pl.ds(base + i, 1), :]
        return c

    lax.fori_loop(0, NB, scatter, 0)
    table_out = pltpu.make_async_copy(table, new_table_ref, sems.at[1])
    table_out.start()

    def unpermute(b, c):
        base = pl.multiple_of(b * BLK, BLK)
        for i in range(BLK):
            looked[pl.ds(base + i, 1), :] = ret_ref[pl.ds(pos_ref[b, i], 1), :]
        return c

    lax.fori_loop(0, NB, unpermute, 0)
    looked_out = pltpu.make_async_copy(looked, looked_ref, sems.at[2])
    looked_out.start()
    accum_out.wait()
    table_out.wait()
    looked_out.wait()


VM = pl.BlockSpec(memory_space=pltpu.VMEM)
SM = pl.BlockSpec(memory_space=pltpu.SMEM)
HBM = pl.BlockSpec(memory_space=pltpu.HBM)


def on_device(lookup_ids, grad_rows, emb_table, row_accum):
    dma = pltpu.SemaphoreType.DMA
    f32 = lambda *s: jax.ShapeDtypeStruct(s, F32)
    smem = lambda *s: pltpu.SMEM(s, I32)
    vmem = lambda *s: pltpu.VMEM(s, F32)
    in_hbm = lambda a: pltpu.with_memory_space_constraint(a, pltpu.HBM)
    ret, upd, rows, pos, stepped, held = pl.pallas_call(
        exchange_kernel,
        out_shape=(f32(LOOK, W), f32(LOOK, W), smem(NB, BLK), smem(NB, BLK), f32(N, BLK), vmem(ROWS, W)),
        in_specs=[HBM, HBM, HBM, HBM],
        out_specs=(VM, VM, SM, SM, VM, VM),
        scratch_shapes=[
            pltpu.VMEM((NB, BLK), I32),
            pltpu.VMEM((NB, BLK), I32),
            pltpu.VMEM((SB, 2 * W), F32),
            pltpu.VMEM((NB, BLK), I32),
            pltpu.VMEM((LOOK, W), F32),
            pltpu.VMEM((N, BLK), F32),
            pltpu.VMEM((LOOK, W), F32),
            pltpu.VMEM((LOOK, W), F32),
            pltpu.VMEM((N, 8, W), I32),
            pltpu.VMEM((N, 8, W), I32),
            pltpu.VMEM((LOOK, 2 * W), BF16),
            pltpu.VMEM((LOOK, LOOK), BF16),
            pltpu.VMEM((LOOK, W), F32),
            pltpu.VMEM((LOOK, W), F32),
            pltpu.VMEM((LOOK, W), F32),
            pltpu.VMEM((N, BLK), F32),
            pltpu.VMEM((LOOK, W), F32),
            dma, dma, dma, pltpu.SemaphoreType.DMA((NSB,)), dma, dma,
            pltpu.SemaphoreType.DMA((2,)), pltpu.SemaphoreType.DMA((4,)),
        ],
        compiler_params=pltpu.CompilerParams(
            collective_id=0, has_side_effects=True, vmem_limit_bytes=28 * 1024 * 1024
        ),
    )(*map(in_hbm, (lookup_ids.reshape(NB, BLK), grad_rows, row_accum.reshape(N, BLK), emb_table)))
    new_table, looked_up, new_accum, _ = pl.pallas_call(
        place_kernel,
        out_shape=(f32(ROWS, W), f32(LOOK, W), f32(N, BLK), vmem(ROWS, W)),
        in_specs=[VM, VM, VM, SM, SM, VM],
        out_specs=(HBM, HBM, HBM, VM),
        input_output_aliases={0: 3},
        scratch_shapes=[pltpu.VMEM((LOOK, W), F32), pltpu.SemaphoreType.DMA((3,))],
        compiler_params=pltpu.CompilerParams(vmem_limit_bytes=4 * 1024 * 1024),
    )(held, upd, ret, rows, pos, stepped)
    return (new_table, new_accum.reshape(ROWS), looked_up)


def solution(mesh):
    in_specs = (P("shard"), P("shard", None), P("shard", None), P("shard"))
    out_specs = (P("shard", None), P("shard"), P("shard", None))
    return jax.shard_map(
        on_device, mesh=mesh, in_specs=in_specs, out_specs=out_specs, check_vma=False
    )
```

```python
import functools

import jax
import jax.numpy as jnp
from jax import lax
from jax.experimental import pallas as pl
from jax.experimental.pallas import tpu as pltpu
from jax.sharding import PartitionSpec as P

LEARNING_RATE = 0.5
EPSILON = 1e-08

MESH = pl.DeviceIdType.MESH
N = 128
W = 128
PER = 16
LOOK = N * PER
ROWS = 16384
ROW_BITS = 14
BLK = 128
NB = LOOK // BLK
SB = 256
NSB = LOOK // SB
PEERS_SB = SB // PER
F32, BF16, I32 = jnp.float32, jnp.bfloat16, jnp.int32


def iota(shape, dim):
    return lax.broadcasted_iota(I32, shape, dim)


def split2(x):
    hi = x.astype(BF16)
    return hi, (x - hi.astype(F32)).astype(BF16)


def onehot(mask):
    return jnp.where(mask, 1.0, 0.0).astype(BF16)


def mm(a, b):
    return jnp.dot(a, b, preferred_element_type=F32)


def mm_nt(a, b):
    return lax.dot_general(a, b, (((1,), (1,)), ((), ())), preferred_element_type=F32)


def hops(k):
    return sum((0, 1, 2, 1)[(k >> i) & 3] for i in (1, 3, 5))


OFFSETS = sorted(range(1, N), key=lambda k: (-hops(k), -(k & 1), k >> 5)) + [0]
SELF = N - 1
PICK = 512
PIECES = 8
EARLY = 2


def remote(src, dst, ssem, rsem, device):
    return pltpu.make_async_remote_copy(
        src_ref=src, dst_ref=dst, send_sem=ssem, recv_sem=rsem, device_id=(device,), device_id_type=MESH
    )


def exchange_kernel(
    ids_hbm, grads_hbm, accum_hbm, table_hbm,
    ret_ref, upd_ref, rows_smem, pos_smem, new_accum_ref, table,
    rows_ref, pos_ref, first, ids_ref, grads_ref, accum_ref, sendbuf, recvbuf, id_send, id_recv, split, eq, emb, rcol, acc_col, start_at,
    msq_col,
    id_ssem, id_rsem, g_ssem, g_rsem, r_ssem, r_rsem, smem_sem, in_sem,
):
    me = lax.axis_index("shard")
    barrier = pltpu.get_barrier_semaphore()

    for k in OFFSETS[:SELF]:
        pl.semaphore_signal(barrier, inc=1, device_id=(me ^ k,), device_id_type=MESH)

    copies = [
        pltpu.make_async_copy(frm, to, in_sem.at[i])
        for i, (frm, to) in enumerate(
            ((ids_hbm, ids_ref), (grads_hbm, grads_ref), (accum_hbm, accum_ref), (table_hbm, table))
        )
    ]
    for copy in copies[:3]:
        copy.start()

    sub = iota((N, BLK), 0)
    lane = iota((N, BLK), 1)
    upper = onehot(sub <= lane)
    for k in range(N):
        start_at[k : k + 1, :] = jnp.full((1, BLK), float(OFFSETS.index(k) * PER - 1), F32)
    copies[0].wait()
    carry = start_at[...]
    for b in range(NB):
        peer = lax.shift_right_logical(ids_ref[b : b + 1, :], ROW_BITS) ^ me
        own = jnp.where(sub == peer, 1.0, 0.0)
        place = mm(own.astype(BF16), upper) + carry
        carry = carry + jnp.sum(own, axis=1, keepdims=True)
        pos_ref[b : b + 1, :] = jnp.sum(own * place, axis=0, keepdims=True).astype(I32)

    def pack_ids():
        w_hi = jnp.zeros((N, BLK), F32)
        w_lo = jnp.zeros((N, BLK), F32)
        for b in range(NB):
            pos = pos_ref[b : b + 1, :]
            row = ids_ref[b : b + 1, :] & (ROWS - 1)
            own = onehot(sub == lax.shift_right_logical(pos, 4))
            here = (sub & (PER - 1)) == (pos & (PER - 1))
            q_hi = jnp.where(here, (row >> 7).astype(F32), 0.0).astype(BF16)
            q_lo = jnp.where(here, (row & 127).astype(F32), 0.0).astype(BF16)
            w_hi = w_hi + mm_nt(own, q_hi)
            w_lo = w_lo + mm_nt(own, q_lo)
        w = (w_hi.astype(I32) << 7) + w_lo.astype(I32)
        for d in range(N):
            id_send[d, 0:1, :] = w[d : d + 1, :]

    copies[1].wait()
    copies[3].start()

    def split_grads(b, c):
        at = pl.ds(pl.multiple_of(b * SB, SB), SB)
        hi, lo = split2(grads_ref[at, :])
        split[at, 0:W] = hi
        split[at, W : 2 * W] = lo
        return c

    lax.fori_loop(0, NSB, split_grads, 0)

    def arrange(t):
        base = pl.multiple_of(t * SB, SB)
        want = iota((SB, BLK), 0) + base
        total = jnp.zeros((SB, 2 * W), F32)
        for b in range(NB):
            pick = onehot(want == pos_ref[b : b + 1, :])
            total = total + mm(pick, split[b * BLK : (b + 1) * BLK, :])
        sendbuf[pl.ds(base, SB), :] = total[:, 0:W] + total[:, W : 2 * W]

    def send_block(t, frm, to, ssem, rsem):
        for q in range(PEERS_SB):
            slot = t * PEERS_SB + q
            if slot != SELF:
                remote(frm(slot), to(slot), ssem, rsem, me ^ OFFSETS[slot]).start()

    def send_block_at(t, *how):
        for block in range(NSB):

            @pl.when(t == block)
            def _():
                send_block(block, *how)

    def slot_rows(ref):
        return lambda slot: ref.at[pl.ds(slot * PER, PER)]

    id_row = lambda ref: lambda slot: ref.at[slot, pl.ds(0, 1)]

    def arrange_only(t, c):
        arrange(t)
        return c

    def arrange_send(t, c):
        arrange(t)
        send_block_at(t, slot_rows(sendbuf), slot_rows(recvbuf), g_ssem, g_rsem.at[t])
        return c

    pack_ids()
    lax.fori_loop(0, EARLY, arrange_only, 0)
    pl.semaphore_wait(barrier, N - 1)
    send_block(0, slot_rows(sendbuf), slot_rows(recvbuf), g_ssem, g_rsem.at[0])
    for t in range(NSB):
        send_block(t, id_row(id_send), id_row(id_recv), id_ssem, id_rsem)
    for t in range(1, EARLY):
        send_block(t, slot_rows(sendbuf), slot_rows(recvbuf), g_ssem, g_rsem.at[t])
    lax.fori_loop(EARLY, NSB, arrange_send, 0)
    id_recv[SELF, 0:1, :] = id_send[SELF, 0:1, :]
    recvbuf[SELF * PER :, :] = sendbuf[SELF * PER :, :]
    to_smem = [
        pltpu.make_async_copy(frm, to, smem_sem.at[i])
        for i, (frm, to) in enumerate(((pos_ref, pos_smem), (rows_ref, rows_smem)))
    ]
    to_smem[0].start()

    ids_all = remote(
        id_send.at[pl.ds(0, N - 1), pl.ds(0, 1)], id_recv.at[pl.ds(0, N - 1), pl.ds(0, 1)], id_ssem, id_rsem, me
    )
    ids_all.wait_send()
    ids_all.wait_recv()
    keep = (iota((8, BLK), 0) & 7) == (iota((8, BLK), 1) >> 4)
    for b in range(NB):
        got = jnp.concatenate([id_recv[8 * b + i, 0:1, :] for i in range(8)], axis=0)
        rows_ref[b : b + 1, :] = jnp.sum(jnp.where(keep, got, 0), axis=0, keepdims=True)
    to_smem[1].start()
    for b in range(NB):
        row = rows_ref[b : b + 1, :].astype(F32)
        rcol[b * BLK : (b + 1) * BLK, :] = jnp.transpose(jnp.broadcast_to(row, (BLK, BLK)))

    copies[2].wait()
    def build(b, c):
        at = pl.ds(pl.multiple_of(b * BLK, BLK), BLK)
        col = rcol[at, :]
        for o in range(NB):
            same = jnp.where(col == rows_ref[o : o + 1, :].astype(F32), 1.0, 0.0)
            eq[at, o * BLK : (o + 1) * BLK] = same.astype(BF16)
        return c

    lax.fori_loop(0, NB, build, 0)

    acc_hi, acc_rest = split2(accum_ref[...])
    acc_lo = (accum_ref[...] - acc_hi.astype(F32) - acc_rest.astype(F32)).astype(BF16)
    acc3 = jnp.concatenate([acc_hi, acc_rest, acc_lo], axis=1)

    def pick_accum(b, c):
        at = pl.ds(pl.multiple_of(b * PICK, PICK), PICK)
        num = rcol[at, :].astype(I32)
        lanes = iota((PICK, BLK), 1)
        picked = mm(onehot((num >> 7) == lanes), acc3)
        picked = picked[:, 0:W] + picked[:, W : 2 * W] + picked[:, 2 * W :]
        acc = jnp.sum(jnp.where((num & 127) == lanes, picked, 0.0), axis=1, keepdims=True)
        acc_col[at, :] = jnp.broadcast_to(acc, (PICK, BLK))
        return c

    lax.fori_loop(0, LOOK // PICK, pick_accum, 0)

    copies[3].wait()
    to_smem[0].wait()
    to_smem[1].wait()

    def gather(t):
        for h in range(SB // BLK):
            base = pl.multiple_of(t * SB + h * BLK, BLK)
            for i in range(BLK):
                r = rows_smem[t * (SB // BLK) + h, i] & (ROWS - 1)
                emb[pl.ds(base + i, 1), :] = table[pl.ds(r, 1), :]

    gather(0)

    def split_recv(t):
        at = pl.ds(pl.multiple_of(t * SB, SB), SB)
        hi, lo = split2(recvbuf[at, :])
        split[at, 0:W] = hi
        split[at, W : 2 * W] = lo
        return mm(eq[0:SB, at], split[at, :])

    def arrived(lo, rows, sem):
        at = pl.ds(lo, rows)
        remote(sendbuf.at[at], recvbuf.at[at], g_ssem, sem, me).wait_recv()

    arrived(0, SB, g_rsem.at[0])
    first[...] = split_recv(0)

    def take(t, c):
        arrived(pl.multiple_of(t * SB, SB), SB, g_rsem.at[t])
        first[...] += split_recv(t)
        return c

    lax.fori_loop(1, NSB - 1, take, 0)
    arrived((NSB - 1) * SB, SB - PER, g_rsem.at[NSB - 1])
    first[...] += split_recv(NSB - 1)

    def update(t, both):
        at = pl.ds(pl.multiple_of(t * SB, SB), SB)
        summed = both[:, 0:W] + both[:, W : 2 * W]
        msq = jnp.broadcast_to(jnp.sum(summed * summed, axis=1, keepdims=True), (SB, W)) * (1.0 / W)
        msq_col[at, :] = msq
        upd_ref[at, :] = emb[at, :] - LEARNING_RATE * summed / (jnp.sqrt(acc_col[at, :] + msq) + EPSILON)

    def update_send(t, c):
        gather(t)
        update(t, mm(eq[pl.ds(pl.multiple_of(t * SB, SB), SB), :], split[...]))
        send_block_at(t, slot_rows(upd_ref), slot_rows(ret_ref), r_ssem, r_rsem)
        return c

    update(0, first[...])
    send_block(0, slot_rows(upd_ref), slot_rows(ret_ref), r_ssem, r_rsem)
    lax.fori_loop(1, NSB, update_send, 0)
    ret_ref[SELF * PER :, :] = upd_ref[SELF * PER :, :]

    delta = jnp.zeros((N, BLK), F32)
    for b in range(NB):
        at = slice(b * BLK, (b + 1) * BLK)
        lo_row = rcol[at, :].astype(I32) & 127
        count = mm(eq[at, :], jnp.ones((LOOK, BLK), BF16))
        term = jnp.where(lo_row == lane, msq_col[at, :] / count, 0.0)
        t_hi, t_mid = split2(term)
        t_lo = (term - t_hi.astype(F32) - t_mid.astype(F32)).astype(BF16)
        pick = onehot((rows_ref[b : b + 1, :] >> 7) == sub)
        delta = delta + mm(pick, t_hi) + mm(pick, t_mid) + mm(pick, t_lo)
    new_accum_ref[...] = accum_ref[...] + delta

    many = pl.ds(0, (N - 1) * PER)
    remote(sendbuf.at[many], recvbuf.at[many], g_ssem, g_rsem.at[0], me).wait_send()
    back = remote(upd_ref.at[many], ret_ref.at[many], r_ssem, r_rsem, me)
    back.wait_send()
    back.wait_recv()


def place_kernel(
    table_ref, upd_ref, ret_ref, rows_ref, pos_ref, accum_ref,
    new_table_ref, looked_ref, new_accum_ref, table,
    looked, sems,
):
    accum_out = pltpu.make_async_copy(accum_ref, new_accum_ref, sems.at[0])
    accum_out.start()

    def scatter(b, c):
        base = pl.multiple_of(b * BLK, BLK)
        for i in range(BLK):
            table[pl.ds(rows_ref[b, i], 1), :] = upd_ref[pl.ds(base + i, 1), :]
        return c

    lax.fori_loop(0, NB, scatter, 0)
    table_out = []
    for i in range(PIECES):
        at = pl.ds(i * (ROWS // PIECES), ROWS // PIECES)
        table_out.append(pltpu.make_async_copy(table.at[at], new_table_ref.at[at], sems.at[2 + i]))
        table_out[-1].start()

    def unpermute(b, c):
        base = pl.multiple_of(b * BLK, BLK)
        for i in range(BLK):
            looked[pl.ds(base + i, 1), :] = ret_ref[pl.ds(pos_ref[b, i], 1), :]
        return c

    lax.fori_loop(0, NB, unpermute, 0)
    looked_out = pltpu.make_async_copy(looked, looked_ref, sems.at[1])
    looked_out.start()
    accum_out.wait()
    for piece in table_out:
        piece.wait()
    looked_out.wait()


VM = pl.BlockSpec(memory_space=pltpu.VMEM)
SM = pl.BlockSpec(memory_space=pltpu.SMEM)
HBM = pl.BlockSpec(memory_space=pltpu.HBM)


def on_device(lookup_ids, grad_rows, emb_table, row_accum):
    dma = pltpu.SemaphoreType.DMA
    f32 = lambda *s: jax.ShapeDtypeStruct(s, F32)
    smem = lambda *s: pltpu.SMEM(s, I32)
    vmem = lambda *s: pltpu.VMEM(s, F32)
    in_hbm = lambda a: pltpu.with_memory_space_constraint(a, pltpu.HBM)
    ret, upd, rows, pos, stepped, held = pl.pallas_call(
        exchange_kernel,
        out_shape=(f32(LOOK, W), f32(LOOK, W), smem(NB, BLK), smem(NB, BLK), f32(N, BLK), vmem(ROWS, W)),
        in_specs=[HBM, HBM, HBM, HBM],
        out_specs=(VM, VM, SM, SM, VM, VM),
        scratch_shapes=[
            pltpu.VMEM((NB, BLK), I32),
            pltpu.VMEM((NB, BLK), I32),
            pltpu.VMEM((SB, 2 * W), F32),
            pltpu.VMEM((NB, BLK), I32),
            pltpu.VMEM((LOOK, W), F32),
            pltpu.VMEM((N, BLK), F32),
            pltpu.VMEM((LOOK, W), F32),
            pltpu.VMEM((LOOK, W), F32),
            pltpu.VMEM((N, 8, W), I32),
            pltpu.VMEM((N, 8, W), I32),
            pltpu.VMEM((LOOK, 2 * W), BF16),
            pltpu.VMEM((LOOK, LOOK), BF16),
            pltpu.VMEM((LOOK, W), F32),
            pltpu.VMEM((LOOK, W), F32),
            pltpu.VMEM((LOOK, W), F32),
            pltpu.VMEM((N, BLK), F32),
            pltpu.VMEM((LOOK, W), F32),
            dma, dma, dma, pltpu.SemaphoreType.DMA((NSB,)), dma, dma,
            pltpu.SemaphoreType.DMA((2,)), pltpu.SemaphoreType.DMA((4,)),
        ],
        compiler_params=pltpu.CompilerParams(
            collective_id=0, has_side_effects=True, vmem_limit_bytes=28 * 1024 * 1024
        ),
    )(*map(in_hbm, (lookup_ids.reshape(NB, BLK), grad_rows, row_accum.reshape(N, BLK), emb_table)))
    new_table, looked_up, new_accum, _ = pl.pallas_call(
        place_kernel,
        out_shape=(f32(ROWS, W), f32(LOOK, W), f32(N, BLK), vmem(ROWS, W)),
        in_specs=[VM, VM, VM, SM, SM, VM],
        out_specs=(HBM, HBM, HBM, VM),
        input_output_aliases={0: 3},
        scratch_shapes=[pltpu.VMEM((LOOK, W), F32), pltpu.SemaphoreType.DMA((2 + PIECES,))],
        compiler_params=pltpu.CompilerParams(vmem_limit_bytes=4 * 1024 * 1024),
    )(held, upd, ret, rows, pos, stepped)
    return (new_table, new_accum.reshape(ROWS), looked_up)


def solution(mesh):
    in_specs = (P("shard"), P("shard", None), P("shard", None), P("shard"))
    out_specs = (P("shard", None), P("shard"), P("shard", None))
    return jax.shard_map(
        on_device, mesh=mesh, in_specs=in_specs, out_specs=out_specs, check_vma=False
    )
```

```python
import functools

import jax
import jax.numpy as jnp
from jax import lax
from jax.experimental import pallas as pl
from jax.experimental.pallas import tpu as pltpu
from jax.sharding import PartitionSpec as P

LEARNING_RATE = 0.5
EPSILON = 1e-08

MESH = pl.DeviceIdType.MESH
N = 128
W = 128
PER = 16
LOOK = N * PER
ROWS = 16384
ROW_BITS = 14
BLK = 128
NB = LOOK // BLK
SB = 256
NSB = LOOK // SB
PEERS_SB = SB // PER
F32, BF16, I32 = jnp.float32, jnp.bfloat16, jnp.int32


def iota(shape, dim):
    return lax.broadcasted_iota(I32, shape, dim)


def split2(x):
    hi = x.astype(BF16)
    return hi, (x - hi.astype(F32)).astype(BF16)


def onehot(mask):
    return jnp.where(mask, 1.0, 0.0).astype(BF16)


def mm(a, b):
    return jnp.dot(a, b, preferred_element_type=F32)


def mm_nt(a, b):
    return lax.dot_general(a, b, (((1,), (1,)), ((), ())), preferred_element_type=F32)


def hops(k):
    return sum((0, 1, 2, 1)[(k >> i) & 3] for i in (1, 3, 5))


OFFSETS = sorted(range(1, N), key=lambda k: (-hops(k), -(k & 1), k >> 5)) + [0]
SELF = N - 1
PICK = 512
PIECES = 8
AHEAD = 4
EARLY = 2


def remote(src, dst, ssem, rsem, device):
    return pltpu.make_async_remote_copy(
        src_ref=src, dst_ref=dst, send_sem=ssem, recv_sem=rsem, device_id=(device,), device_id_type=MESH
    )


def exchange_kernel(
    ids_hbm, grads_hbm, accum_hbm, table_hbm,
    ret_ref, upd_ref, rows_smem, pos_smem, new_accum_ref, table,
    rows_ref, pos_ref, first, ids_ref, grads_ref, accum_ref, sendbuf, recvbuf, id_send, id_recv, split, eq, emb, rcol, acc_col, start_at,
    msq_col,
    id_ssem, id_rsem, g_ssem, g_rsem, r_ssem, r_rsem, smem_sem, in_sem,
):
    me = lax.axis_index("shard")
    barrier = pltpu.get_barrier_semaphore()

    for k in OFFSETS[:SELF]:
        pl.semaphore_signal(barrier, inc=1, device_id=(me ^ k,), device_id_type=MESH)

    copies = [
        pltpu.make_async_copy(frm, to, in_sem.at[i])
        for i, (frm, to) in enumerate(
            ((ids_hbm, ids_ref), (grads_hbm, grads_ref), (accum_hbm, accum_ref), (table_hbm, table))
        )
    ]
    for copy in copies[:3]:
        copy.start()

    sub = iota((N, BLK), 0)
    lane = iota((N, BLK), 1)
    upper = onehot(sub <= lane)
    for k in range(N):
        start_at[k : k + 1, :] = jnp.full((1, BLK), float(OFFSETS.index(k) * PER - 1), F32)
    copies[0].wait()
    carry = start_at[...]
    for b in range(NB):
        peer = lax.shift_right_logical(ids_ref[b : b + 1, :], ROW_BITS) ^ me
        own = jnp.where(sub == peer, 1.0, 0.0)
        place = mm(own.astype(BF16), upper) + carry
        carry = carry + jnp.sum(own, axis=1, keepdims=True)
        pos_ref[b : b + 1, :] = jnp.sum(own * place, axis=0, keepdims=True).astype(I32)

    def pack_ids():
        w_hi = jnp.zeros((N, BLK), F32)
        w_lo = jnp.zeros((N, BLK), F32)
        for b in range(NB):
            pos = pos_ref[b : b + 1, :]
            row = ids_ref[b : b + 1, :] & (ROWS - 1)
            own = onehot(sub == lax.shift_right_logical(pos, 4))
            here = (sub & (PER - 1)) == (pos & (PER - 1))
            q_hi = jnp.where(here, (row >> 7).astype(F32), 0.0).astype(BF16)
            q_lo = jnp.where(here, (row & 127).astype(F32), 0.0).astype(BF16)
            w_hi = w_hi + mm_nt(own, q_hi)
            w_lo = w_lo + mm_nt(own, q_lo)
        w = (w_hi.astype(I32) << 7) + w_lo.astype(I32)
        for d in range(N):
            id_send[d, 0:1, :] = w[d : d + 1, :]

    copies[1].wait()
    copies[3].start()

    def split_grads(b, c):
        at = pl.ds(pl.multiple_of(b * SB, SB), SB)
        hi, lo = split2(grads_ref[at, :])
        split[at, 0:W] = hi
        split[at, W : 2 * W] = lo
        return c

    lax.fori_loop(0, NSB, split_grads, 0)

    def arrange(t):
        base = pl.multiple_of(t * SB, SB)
        want = iota((SB, BLK), 0) + base
        total = jnp.zeros((SB, 2 * W), F32)
        for b in range(NB):
            pick = onehot(want == pos_ref[b : b + 1, :])
            total = total + mm(pick, split[b * BLK : (b + 1) * BLK, :])
        sendbuf[pl.ds(base, SB), :] = total[:, 0:W] + total[:, W : 2 * W]

    def send_block(t, frm, to, ssem, rsem):
        for q in range(PEERS_SB):
            slot = t * PEERS_SB + q
            if slot != SELF:
                remote(frm(slot), to(slot), ssem, rsem, me ^ OFFSETS[slot]).start()

    def send_block_at(t, *how):
        for block in range(NSB):

            @pl.when(t == block)
            def _():
                send_block(block, *how)

    def slot_rows(ref):
        return lambda slot: ref.at[pl.ds(slot * PER, PER)]

    id_row = lambda ref: lambda slot: ref.at[slot, pl.ds(0, 1)]

    def arrange_only(t, c):
        arrange(t)
        return c

    def arrange_send(t, c):
        arrange(t)
        send_block_at(t, slot_rows(sendbuf), slot_rows(recvbuf), g_ssem, g_rsem.at[t])
        return c

    pack_ids()
    lax.fori_loop(0, EARLY, arrange_only, 0)
    pl.semaphore_wait(barrier, N - 1)
    send_block(0, slot_rows(sendbuf), slot_rows(recvbuf), g_ssem, g_rsem.at[0])
    for t in range(NSB):
        send_block(t, id_row(id_send), id_row(id_recv), id_ssem, id_rsem)
    for t in range(1, EARLY):
        send_block(t, slot_rows(sendbuf), slot_rows(recvbuf), g_ssem, g_rsem.at[t])
    lax.fori_loop(EARLY, NSB, arrange_send, 0)
    id_recv[SELF, 0:1, :] = id_send[SELF, 0:1, :]
    recvbuf[SELF * PER :, :] = sendbuf[SELF * PER :, :]
    to_smem = [
        pltpu.make_async_copy(frm, to, smem_sem.at[i])
        for i, (frm, to) in enumerate(((pos_ref, pos_smem), (rows_ref, rows_smem)))
    ]
    to_smem[0].start()

    ids_all = remote(
        id_send.at[pl.ds(0, N - 1), pl.ds(0, 1)], id_recv.at[pl.ds(0, N - 1), pl.ds(0, 1)], id_ssem, id_rsem, me
    )
    ids_all.wait_send()
    ids_all.wait_recv()
    keep = (iota((8, BLK), 0) & 7) == (iota((8, BLK), 1) >> 4)
    for b in range(NB):
        got = jnp.concatenate([id_recv[8 * b + i, 0:1, :] for i in range(8)], axis=0)
        rows_ref[b : b + 1, :] = jnp.sum(jnp.where(keep, got, 0), axis=0, keepdims=True)
    to_smem[1].start()
    for b in range(NB):
        row = rows_ref[b : b + 1, :].astype(F32)
        rcol[b * BLK : (b + 1) * BLK, :] = jnp.transpose(jnp.broadcast_to(row, (BLK, BLK)))

    copies[2].wait()
    def build(b, c):
        at = pl.ds(pl.multiple_of(b * BLK, BLK), BLK)
        col = rcol[at, :]
        for o in range(NB):
            same = jnp.where(col == rows_ref[o : o + 1, :].astype(F32), 1.0, 0.0)
            eq[at, o * BLK : (o + 1) * BLK] = same.astype(BF16)
        return c

    lax.fori_loop(0, NB, build, 0)

    acc_hi, acc_rest = split2(accum_ref[...])
    acc_lo = (accum_ref[...] - acc_hi.astype(F32) - acc_rest.astype(F32)).astype(BF16)
    acc3 = jnp.concatenate([acc_hi, acc_rest, acc_lo], axis=1)

    def pick_accum(b, c):
        at = pl.ds(pl.multiple_of(b * PICK, PICK), PICK)
        num = rcol[at, :].astype(I32)
        lanes = iota((PICK, BLK), 1)
        picked = mm(onehot((num >> 7) == lanes), acc3)
        picked = picked[:, 0:W] + picked[:, W : 2 * W] + picked[:, 2 * W :]
        acc = jnp.sum(jnp.where((num & 127) == lanes, picked, 0.0), axis=1, keepdims=True)
        acc_col[at, :] = jnp.broadcast_to(acc, (PICK, BLK))
        return c

    lax.fori_loop(0, LOOK // PICK, pick_accum, 0)

    copies[3].wait()
    to_smem[0].wait()
    to_smem[1].wait()

    def gather(t):
        for h in range(SB // BLK):
            base = pl.multiple_of(t * SB + h * BLK, BLK)
            for i in range(BLK):
                r = rows_smem[t * (SB // BLK) + h, i] & (ROWS - 1)
                emb[pl.ds(base + i, 1), :] = table[pl.ds(r, 1), :]

    gather(0)

    def split_recv(t):
        at = pl.ds(pl.multiple_of(t * SB, SB), SB)
        hi, lo = split2(recvbuf[at, :])
        split[at, 0:W] = hi
        split[at, W : 2 * W] = lo
        return mm(eq[0:SB, at], split[at, :])

    def arrived(lo, rows, sem):
        at = pl.ds(lo, rows)
        remote(sendbuf.at[at], recvbuf.at[at], g_ssem, sem, me).wait_recv()

    arrived(0, SB, g_rsem.at[0])
    first[...] = split_recv(0)

    def take(t, c):
        arrived(pl.multiple_of(t * SB, SB), SB, g_rsem.at[t])
        first[...] += split_recv(t)
        return c

    def gather_take(t, c):
        gather(t)
        return take(t, c)

    lax.fori_loop(1, AHEAD, gather_take, 0)
    lax.fori_loop(AHEAD, NSB - 1, take, 0)
    arrived((NSB - 1) * SB, SB - PER, g_rsem.at[NSB - 1])
    first[...] += split_recv(NSB - 1)

    def update(t, both):
        at = pl.ds(pl.multiple_of(t * SB, SB), SB)
        summed = both[:, 0:W] + both[:, W : 2 * W]
        msq = jnp.broadcast_to(jnp.sum(summed * summed, axis=1, keepdims=True), (SB, W)) * (1.0 / W)
        msq_col[at, :] = msq
        upd_ref[at, :] = emb[at, :] - LEARNING_RATE * summed / (jnp.sqrt(acc_col[at, :] + msq) + EPSILON)

    def update_send(t, c):
        update(t, mm(eq[pl.ds(pl.multiple_of(t * SB, SB), SB), :], split[...]))
        send_block_at(t, slot_rows(upd_ref), slot_rows(ret_ref), r_ssem, r_rsem)
        return c

    update(0, first[...])
    send_block(0, slot_rows(upd_ref), slot_rows(ret_ref), r_ssem, r_rsem)
    def gather_update_send(t, c):
        gather(t)
        return update_send(t, c)

    lax.fori_loop(1, AHEAD, update_send, 0)
    lax.fori_loop(AHEAD, NSB, gather_update_send, 0)
    ret_ref[SELF * PER :, :] = upd_ref[SELF * PER :, :]

    delta = jnp.zeros((N, BLK), F32)
    for b in range(NB):
        at = slice(b * BLK, (b + 1) * BLK)
        lo_row = rcol[at, :].astype(I32) & 127
        count = mm(eq[at, :], jnp.ones((LOOK, BLK), BF16))
        term = jnp.where(lo_row == lane, msq_col[at, :] / count, 0.0)
        t_hi, t_mid = split2(term)
        t_lo = (term - t_hi.astype(F32) - t_mid.astype(F32)).astype(BF16)
        pick = onehot((rows_ref[b : b + 1, :] >> 7) == sub)
        delta = delta + mm(pick, t_hi) + mm(pick, t_mid) + mm(pick, t_lo)
    new_accum_ref[...] = accum_ref[...] + delta

    many = pl.ds(0, (N - 1) * PER)
    remote(sendbuf.at[many], recvbuf.at[many], g_ssem, g_rsem.at[0], me).wait_send()
    back = remote(upd_ref.at[many], ret_ref.at[many], r_ssem, r_rsem, me)
    back.wait_send()
    back.wait_recv()


def place_kernel(
    table_ref, upd_ref, ret_ref, rows_ref, pos_ref, accum_ref,
    new_table_ref, looked_ref, new_accum_ref, table,
    looked, sems,
):
    accum_out = pltpu.make_async_copy(accum_ref, new_accum_ref, sems.at[0])
    accum_out.start()

    def scatter(b, c):
        base = pl.multiple_of(b * BLK, BLK)
        for i in range(BLK):
            table[pl.ds(rows_ref[b, i], 1), :] = upd_ref[pl.ds(base + i, 1), :]
        return c

    lax.fori_loop(0, NB, scatter, 0)
    table_out = []
    for i in range(PIECES):
        at = pl.ds(i * (ROWS // PIECES), ROWS // PIECES)
        table_out.append(pltpu.make_async_copy(table.at[at], new_table_ref.at[at], sems.at[2 + i]))
        table_out[-1].start()

    def unpermute(b, c):
        base = pl.multiple_of(b * BLK, BLK)
        for i in range(BLK):
            looked[pl.ds(base + i, 1), :] = ret_ref[pl.ds(pos_ref[b, i], 1), :]
        return c

    lax.fori_loop(0, NB, unpermute, 0)
    looked_out = pltpu.make_async_copy(looked, looked_ref, sems.at[1])
    looked_out.start()
    accum_out.wait()
    for piece in table_out:
        piece.wait()
    looked_out.wait()


VM = pl.BlockSpec(memory_space=pltpu.VMEM)
SM = pl.BlockSpec(memory_space=pltpu.SMEM)
HBM = pl.BlockSpec(memory_space=pltpu.HBM)


def on_device(lookup_ids, grad_rows, emb_table, row_accum):
    dma = pltpu.SemaphoreType.DMA
    f32 = lambda *s: jax.ShapeDtypeStruct(s, F32)
    smem = lambda *s: pltpu.SMEM(s, I32)
    vmem = lambda *s: pltpu.VMEM(s, F32)
    in_hbm = lambda a: pltpu.with_memory_space_constraint(a, pltpu.HBM)
    ret, upd, rows, pos, stepped, held = pl.pallas_call(
        exchange_kernel,
        out_shape=(f32(LOOK, W), f32(LOOK, W), smem(NB, BLK), smem(NB, BLK), f32(N, BLK), vmem(ROWS, W)),
        in_specs=[HBM, HBM, HBM, HBM],
        out_specs=(VM, VM, SM, SM, VM, VM),
        scratch_shapes=[
            pltpu.VMEM((NB, BLK), I32),
            pltpu.VMEM((NB, BLK), I32),
            pltpu.VMEM((SB, 2 * W), F32),
            pltpu.VMEM((NB, BLK), I32),
            pltpu.VMEM((LOOK, W), F32),
            pltpu.VMEM((N, BLK), F32),
            pltpu.VMEM((LOOK, W), F32),
            pltpu.VMEM((LOOK, W), F32),
            pltpu.VMEM((N, 8, W), I32),
            pltpu.VMEM((N, 8, W), I32),
            pltpu.VMEM((LOOK, 2 * W), BF16),
            pltpu.VMEM((LOOK, LOOK), BF16),
            pltpu.VMEM((LOOK, W), F32),
            pltpu.VMEM((LOOK, W), F32),
            pltpu.VMEM((LOOK, W), F32),
            pltpu.VMEM((N, BLK), F32),
            pltpu.VMEM((LOOK, W), F32),
            dma, dma, dma, pltpu.SemaphoreType.DMA((NSB,)), dma, dma,
            pltpu.SemaphoreType.DMA((2,)), pltpu.SemaphoreType.DMA((4,)),
        ],
        compiler_params=pltpu.CompilerParams(
            collective_id=0, has_side_effects=True, vmem_limit_bytes=28 * 1024 * 1024
        ),
    )(*map(in_hbm, (lookup_ids.reshape(NB, BLK), grad_rows, row_accum.reshape(N, BLK), emb_table)))
    new_table, looked_up, new_accum, _ = pl.pallas_call(
        place_kernel,
        out_shape=(f32(ROWS, W), f32(LOOK, W), f32(N, BLK), vmem(ROWS, W)),
        in_specs=[VM, VM, VM, SM, SM, VM],
        out_specs=(HBM, HBM, HBM, VM),
        input_output_aliases={0: 3},
        scratch_shapes=[pltpu.VMEM((LOOK, W), F32), pltpu.SemaphoreType.DMA((2 + PIECES,))],
        compiler_params=pltpu.CompilerParams(vmem_limit_bytes=4 * 1024 * 1024),
    )(held, upd, ret, rows, pos, stepped)
    return (new_table, new_accum.reshape(ROWS), looked_up)


def solution(mesh):
    in_specs = (P("shard"), P("shard", None), P("shard", None), P("shard"))
    out_specs = (P("shard", None), P("shard"), P("shard", None))
    return jax.shard_map(
        on_device, mesh=mesh, in_specs=in_specs, out_specs=out_specs, check_vma=False
    )
```
